32 devices in a mesh: batch: 2 (over x), row: 4 (over z), col: 4 (over y, core).
Axes of the slice: x: 2, y: 2, z: 4, core: 2. Of those that a mesh axis runs over, the one named last changes fastest.
Arguments:
- left_op: bfloat16 [14336, 7168], P(('batch', 'row'), 'col'), parts along dimension 0
- left_start: float32 [14336, 256], P(('batch', 'row', 'col')), parts along dimension 0
- right_op: bfloat16 [4096, 2048], P(('batch', 'row'), 'col'), parts along dimension 0
- right_start: float32 [4096, 256], P(('batch', 'row', 'col')), parts along dimension 0
Outputs:
- output 1: float32 [14336, 256], P(('batch', 'row', 'col')), parts along dimension 0
- output 2: float32 [512, 256], P('batch'), parts along dimension 0
- output 3: float32 [4096, 256], P(('batch', 'row', 'col')), parts along dimension 0
- output 4: float32 [512, 256], P('batch'), parts along dimension 0
There are 2 independent parts. The reference program is written for one: setup_inputs(seed, part) draws one part's arguments, and reference() takes and returns one part's arrays. A program takes and returns all parts, laid end to end along the dimension named above; each array names one.
All inputs are finite; a program needn't handle non-finite values.
Results may differ from the reference program's by a relative error of at most 0.001.
Values are sent between devices in bfloat16 or wider.
A program may use at most 1 GiB of HBM per device.

```python
import jax
import jax.numpy as jnp
from jax import lax

N = 7168
N2 = 2048
S = 256
SWEEPS = 4


def build_operator(key, size):
    key_vec, key_val, key_noise = jax.random.split(key, 3)
    eig_basis = jax.random.normal(key_vec, (size, S), jnp.float32) * (size ** -0.5)
    levels = 1.5 * 4.0 ** jax.random.uniform(key_val, (S,), jnp.float32)
    noise_mat = jax.random.normal(key_noise, (size, size), jnp.float32) * (0.1 * size ** -0.5)
    full_mat = jnp.dot(eig_basis * levels, eig_basis.T) + noise_mat
    symmetric = 0.5 * (full_mat + full_mat.T) + 0.5 * jnp.eye(size, dtype=jnp.float32)
    return symmetric.astype(jnp.bfloat16)


def setup_inputs(seed: int = 0, part: int = 0) -> dict:
    base_key = jax.random.fold_in(jax.random.key(seed), part)
    key_left_op, key_left_start, key_right_op, key_right_start = jax.random.split(base_key, 4)
    return {
        "left_op": build_operator(key_left_op, N),
        "left_start": jax.random.normal(key_left_start, (N, S), jnp.float32),
        "right_op": build_operator(key_right_op, N2),
        "right_start": jax.random.normal(key_right_start, (N2, S), jnp.float32),
    }


def cholqr_step(y_mat, gram_mat):
    chol_low = jnp.linalg.cholesky(gram_mat)
    return lax.linalg.triangular_solve(chol_low, y_mat, left_side=False, lower=True, transpose_a=True)


def orthonormalize(y_mat):
    row_count = y_mat.shape[0]
    y_half = y_mat.astype(jnp.bfloat16)
    gram_one = jnp.dot(y_half.T, y_half, preferred_element_type=jnp.float32) / row_count
    y_one = cholqr_step(y_mat, gram_one)
    gram_two = jnp.dot(y_one.T, y_one, precision=lax.Precision.HIGHEST) / row_count
    return cholqr_step(y_one, gram_two)


def iterate(operator, start_block):
    def one_sweep(x_cur, unused):
        y_mat = jnp.dot(operator, x_cur.astype(jnp.bfloat16), preferred_element_type=jnp.float32)
        return orthonormalize(y_mat), None

    x_final, scan_rest = lax.scan(one_sweep, start_block, None, length=SWEEPS)
    z_mat = jnp.dot(operator, x_final.astype(jnp.bfloat16), preferred_element_type=jnp.float32)
    rayleigh = jnp.dot(x_final.T, z_mat, precision=lax.Precision.HIGHEST) / x_final.shape[0]
    return x_final, rayleigh


def reference(left_op, left_start, right_op, right_start):
    left_basis, left_rayleigh = iterate(left_op, left_start)
    right_basis, right_rayleigh = iterate(right_op, right_start)
    return (left_basis, left_rayleigh, right_basis, right_rayleigh)
```

```python
import jax
import jax.numpy as jnp
from jax import lax
from jax.experimental import pallas as pl
from jax.experimental.pallas import tpu as pltpu
from jax.sharding import PartitionSpec as P

SWEEPS = 4
MESH = pl.DeviceIdType.MESH
HI = lax.Precision.HIGHEST
NB = 32


def dot_hi(a, b, dims):
    return lax.dot_general(a, b, (dims, ((), ())), precision=HI, preferred_element_type=jnp.float32)


def diag_block(blk_l, blk_r, lane0):
    lane = lax.broadcasted_iota(jnp.int32, (NB, 128), 1)
    row = lax.broadcasted_iota(jnp.int32, (NB, 128), 0)
    is_left = (lane // NB) % 2 == 0
    groups = NB // 8
    cols = []
    for g in range(groups):
        r0 = 8 * g
        cols.append(jnp.stack([
            jnp.where(is_left[r0:], blk_l[r0:, lane0 + k:lane0 + k + 1], blk_r[r0:, lane0 + k:lane0 + k + 1])
            for k in range(r0, r0 + 8)]))
    w = jnp.where(lane % NB == row, 1.0, 0.0)
    piv = []
    for j in range(NB):
        g0, jj = divmod(j, 8)
        r0 = 8 * g0
        u = cols[g0][0]
        p = u[jj:jj + 1]
        piv.append(p)
        if j == NB - 1:
            break
        m = jnp.where(row[r0:] > j, u * (1.0 / p), 0.0)
        if jj < 7:
            cols[g0] = cols[g0][1:] - m[None] * u[jj + 1:8][:, None, :]
        for g in range(g0 + 1, groups):
            d = 8 * (g - g0)
            cols[g] = cols[g] - m[d:][None] * u[d:d + 8][:, None, :]
        w_low = w[r0:] - m * w[j:j + 1]
        w = w_low if g0 == 0 else jnp.concatenate([w[:r0], w_low], axis=0)
    return w * lax.rsqrt(jnp.concatenate(piv, axis=0))


def chol_inverse(s, w):
    lane64 = lax.broadcasted_iota(jnp.int32, (NB, 128), 1)
    rowi = lax.broadcasted_iota(jnp.int32, (256, 256), 0)
    lanei = lax.broadcasted_iota(jnp.int32, (256, 256), 1)
    for o in range(2):
        w[o] = jnp.where(rowi == lanei, 1.0, 0.0)
    for h in range(2):
        base = 128 * h
        for b in range(4):
            r0 = base + NB * b
            rows = slice(r0, r0 + NB)
            grp = slice(base, base + 128)
            li = diag_block(s[0, rows, grp], s[1, rows, grp], NB * b)
            lhs = jnp.concatenate([jnp.where(lane64 < NB, li, 0.0), jnp.where((lane64 >= NB) & (lane64 < 2 * NB), li, 0.0)], axis=0)[:, :2 * NB]
            rhs = jnp.concatenate([jnp.concatenate([s[o, rows, base:256], w[o, rows, 0:base + 128]], axis=1) for o in range(2)], axis=0)
            pan = dot_hi(lhs, rhs, ((1,), (0,)))
            ns = 256 - base
            for o in range(2):
                po = pan[NB * o:NB * o + NB]
                s[o, rows, base:256] = po[:, :ns]
                w[o, rows, 0:base + 128] = po[:, ns:]
                if b < 3:
                    pt = po[:, 0:128].T[NB * (b + 1):]
                    upd = dot_hi(pt, po, ((1,), (0,)))
                    rest = slice(r0 + NB, base + 128)
                    s[o, rest, base:256] = s[o, rest, base:256] - upd[:, :ns]
                    w[o, rest, 0:base + 128] = w[o, rest, 0:base + 128] - upd[:, ns:]
        if h == 0:
            for o in range(2):
                pb = s[o, 0:128, 128:256]
                full = jnp.concatenate([pb, w[o, 0:128, 0:128]], axis=1)
                upd = dot_hi(pb.T, full, ((1,), (0,)))
                s[o, 128:256, 128:256] = s[o, 128:256, 128:256] - upd[:, :128]
                w[o, 128:256, 0:128] = w[o, 128:256, 0:128] - upd[:, 128:]


def remote(src, dst, send_sem, recv_sem, row, col):
    return pltpu.make_async_remote_copy(src_ref=src, dst_ref=dst, send_sem=send_sem, recv_sem=recv_sem, device_id={"row": row, "col": col}, device_id_type=MESH)


def place():
    z = lax.axis_index("row")
    c = lax.axis_index("col")
    return z, c, c // 2, c % 2


def entry_barrier():
    z, c, y, core = place()
    barrier = pltpu.get_barrier_semaphore()
    peers = []
    k = z * 2 + y
    for e in range(1, 8):
        q = (k + e) % 8
        peers.append((q // 2, (q % 2) * 2 + core))
    peers.append((z, 2 * y + 1 - core))
    peers.append((z, 2 * (1 - y) + 1 - core))
    for row, col in peers:
        pl.semaphore_signal(barrier, inc=1, device_id={"row": row, "col": col}, device_id_type=MESH)
    pl.semaphore_wait(barrier, len(peers))


def product(ops, xs, ys, bufs):
    z, c, y, core = place()
    xb, zbuf, xcol, zs, zr, cs, cr = bufs["gather"]
    dsend, drecv, ysend, yrecv, ds, dr, yss, yrs = bufs["scatter"]
    partner = 2 * y + 1 - core
    across = 2 * (1 - y) + core

    def gather_copy(o, d):
        return remote(xb[o], zbuf[o].at[d], zs.at[o, d], zr.at[o, d], (z + d) % 4, c)

    def cross_copy(o, d):
        src = xb[o] if d == 0 else zbuf[o].at[d]
        to = (z - d + 4) % 4
        return to, remote(src, xcol[o].at[c], cs.at[o, d], cr.at[o, c], z, to)

    for o in range(2):
        xb[o][...] = xs[o][...].astype(jnp.bfloat16)
    for o in range(2):
        for d in (2, 1, 3):
            gather_copy(o, d).start()
    for d in (0, 1, 3, 2):
        for o in range(2):
            if d:
                gather_copy(o, d).wait_recv()
            to, copy = cross_copy(o, d)

            @pl.when(to != c)
            def _():
                copy.start()

            @pl.when(to == c)
            def _():
                xcol[o][c] = xb[o][...] if d == 0 else zbuf[o][d]

    for o in range(2):
        for e in range(1, 4):
            frm = (c + e) % 4
            remote(xb[o], xcol[o].at[frm], cs.at[o, 0], cr.at[o, frm], z, frm).wait_recv()
        n = xs[o].shape[0]
        full = xcol[o][...].reshape(4 * n, 256)

        def part(q):
            return jnp.dot(ops[o][pl.ds(pl.multiple_of(q * n, n), n), :], full, preferred_element_type=jnp.float32)

        def d2d(i):
            return remote(dsend[o].at[i], drecv[o].at[i], ds.at[o, i], dr.at[o, i], z, partner)

        dsend[o][0] = part(2 * (1 - y) + 1 - core)
        d2d(0).start()
        mine = part(2 * (1 - y) + core)
        d2d(0).wait_recv()
        ysend[o][...] = mine + drecv[o][0]
        remote(ysend[o], yrecv[o], yss.at[o], yrs.at[o], z, across).start()
        dsend[o][1] = part(2 * y + 1 - core)
        d2d(1).start()
        mine = part(2 * y + core)
        d2d(1).wait_recv()
        ys[o][...] = mine + drecv[o][1]
    for o in (1, 0):
        hop = remote(ysend[o], yrecv[o], yss.at[o], yrs.at[o], z, across)
        hop.wait_recv()
        ys[o][...] = ys[o][...] + yrecv[o][...]
        hop.wait_send()
        for i in range(2):
            remote(dsend[o].at[i], drecv[o].at[i], ds.at[o, i], dr.at[o, i], z, partner).wait_send()
        for d in range(1, 4):
            gather_copy(o, d).wait_send()
        for d in range(4):
            to, copy = cross_copy(o, d)

            @pl.when(to != c)
            def _():
                copy.wait_send()


def all_sum(half, bufs):
    z, c, y, core = place()
    gp, r1, acc, r2, res, s1, s2, s3, s4, v1, v2, v3, v4 = bufs["sum"]
    partner = 2 * y + 1 - core
    piece = half // 8
    k = z * 2 + y

    def peer(e):
        q = (k + e) % 8
        return q, q // 2, (q % 2) * 2 + core

    one = remote(gp.at[1 - core, pl.ds(0, half)], r1.at[pl.ds(0, half)], s1, v1, z, partner)
    one.start()
    one.wait_recv()
    acc[0:half] = gp[core, 0:half] + r1[0:half]

    def spread(e):
        q, row, col = peer(e)
        return remote(acc.at[pl.ds(pl.multiple_of(q * piece, piece), piece)], r2.at[e, pl.ds(0, piece)], s2.at[e], v2.at[e], row, col)

    order = (4, 3, 5, 2, 6, 1, 7)
    for e in order:
        spread(e).start()
    mine = pl.ds(pl.multiple_of(k * piece, piece), piece)
    total = acc[mine]
    for e in range(1, 8):
        spread(e).wait_recv()
        total = total + r2[e, 0:piece]
    res[core, mine] = total

    def share(e, slot):
        q, row, col = peer(e)
        at = pl.ds(pl.multiple_of(slot * piece, piece), piece)
        return remote(res.at[core, at], res.at[core, at], s3.at[e], v3.at[e], row, col)

    for e in order:
        share(e, k).start()
    for e in range(1, 8):
        share(e, (k + 8 - e) % 8).wait_recv()
    last = remote(res.at[core, pl.ds(0, half)], res.at[core, pl.ds(0, half)], s4, v4, z, partner)
    last.start()
    got = remote(res.at[1 - core, pl.ds(0, half)], res.at[1 - core, pl.ds(0, half)], s4, v4, z, partner)
    got.wait_recv()
    one.wait_send()
    for e in range(1, 8):
        spread(e).wait_send()
        share(e, k).wait_send()
    last.wait_send()


def pack_gram(mats, precision, gp):
    for o in range(2):
        g = lax.dot_general(mats[o], mats[o], (((0,), (0,)), ((), ())), precision=precision, preferred_element_type=jnp.float32)
        gp[o, 0:128] = g[0:128, 0:128]
        gp[o, 128:256] = g[0:128, 128:256]
        gp[o, 256:384] = g[128:256, 128:256]


def body(lop, lx, rop, rx, xl_out, hl_out, xr_out, hr_out, lv, rv, xl, xr, yl, yr, s, w, *rest):
    names = iter(rest)

    def take(n):
        return [next(names) for _ in range(n)]

    xb, zbuf, xcol = take(2), take(2), take(2)
    gsems = take(4)
    dsend, drecv, ysend, yrecv = take(2), take(2), take(2), take(2)
    ssems = take(4)
    bufs = {"gather": (xb, zbuf, xcol, *gsems), "scatter": (dsend, drecv, ysend, yrecv, *ssems), "sum": take(13)}
    (lsem,) = take(1)
    loads = [pltpu.make_async_copy(lop, lv, lsem.at[0]), pltpu.make_async_copy(rop, rv, lsem.at[1])]
    for load in loads:
        load.start()
    xs, ys, ops = (xl, xr), (yl, yr), (lv, rv)
    scales = [1.0 / (16 * ref.shape[0]) for ref in xs]
    xl[...] = lx[...]
    xr[...] = rx[...]
    entry_barrier()
    for load in loads:
        load.wait()

    gp, res = bufs["sum"][0], bufs["sum"][4]

    def half_step(phase, carry):
        @pl.when(phase == 0)
        def _():
            pack_gram([r[...].astype(jnp.bfloat16) for r in ys], None, gp)

        @pl.when(phase == 1)
        def _():
            pack_gram([r[...] for r in ys], HI, gp)

        all_sum(384, bufs)
        for o in range(2):
            s[o, 0:128, 0:128] = res[o, 0:128] * scales[o]
            s[o, 0:128, 128:256] = res[o, 128:256] * scales[o]
            s[o, 128:256, 128:256] = res[o, 256:384] * scales[o]
        chol_inverse(s, w)
        for o in range(2):
            ys[o][...] = dot_hi(ys[o][...], w[o], ((1,), (1,)))
        return carry

    def sweep(i, carry):
        product(ops, xs, ys, bufs)
        lax.fori_loop(0, 2, half_step, 0)
        for o in range(2):
            xs[o][...] = ys[o][...]
        return carry

    lax.fori_loop(0, SWEEPS, sweep, 0)
    product(ops, xs, ys, bufs)
    for o in range(2):
        h = dot_hi(xs[o][...], ys[o][...], ((0,), (0,)))
        gp[o, 0:256] = h[:, 0:128]
        gp[o, 256:512] = h[:, 128:256]
    all_sum(512, bufs)
    for o, out in enumerate((hl_out, hr_out)):
        out[:, 0:128] = res[o, 0:256] * scales[o]
        out[:, 128:256] = res[o, 256:512] * scales[o]
    xl_out[...] = xl[...]
    xr_out[...] = xr[...]


def solution(mesh):
    f32, bf16 = jnp.float32, jnp.bfloat16

    def local_program(left_op, left_start, right_op, right_start):
        nl, nr = left_start.shape[0], right_start.shape[0]
        vm = pl.BlockSpec(memory_space=pltpu.VMEM)
        hbm = pl.BlockSpec(memory_space=pl.ANY)
        dma = pltpu.SemaphoreType.DMA

        def pair(shape, dtype):
            return [pltpu.VMEM(shape(nl), dtype), pltpu.VMEM(shape(nr), dtype)]

        scratch = [pltpu.VMEM(left_op.shape, bf16), pltpu.VMEM(right_op.shape, bf16)]
        scratch += pair(lambda n: (n, 256), f32) + pair(lambda n: (n, 256), f32)
        scratch += [pltpu.VMEM((2, 256, 256), f32), pltpu.VMEM((2, 256, 256), f32)]
        scratch += pair(lambda n: (n, 256), bf16) + pair(lambda n: (4, n, 256), bf16) + pair(lambda n: (4, n, 256), bf16)
        scratch += [dma((2, 4)), dma((2, 4)), dma((2, 4)), dma((2, 4))]
        scratch += pair(lambda n: (2, n, 256), f32) + pair(lambda n: (2, n, 256), f32)
        scratch += pair(lambda n: (n, 256), f32) + pair(lambda n: (n, 256), f32)
        scratch += [dma((2, 2)), dma((2, 2)), dma((2,)), dma((2,))]
        scratch += [pltpu.VMEM((2, 512, 128), f32), pltpu.VMEM((512, 128), f32), pltpu.VMEM((512, 128), f32), pltpu.VMEM((8, 64, 128), f32), pltpu.VMEM((2, 512, 128), f32)]
        scratch += [dma, dma((8,)), dma((8,)), dma, dma, dma((8,)), dma((8,)), dma]
        scratch += [dma((2,))]
        small = jax.ShapeDtypeStruct((256, 256), f32)
        xl, hl, xr, hr = pl.pallas_call(
            body,
            out_shape=(jax.ShapeDtypeStruct((nl, 256), f32), small, jax.ShapeDtypeStruct((nr, 256), f32), small),
            in_specs=[hbm, vm, hbm, vm],
            out_specs=(vm, vm, vm, vm),
            scratch_shapes=scratch,
            compiler_params=pltpu.CompilerParams(collective_id=0, has_side_effects=True, vmem_limit_bytes=60 * 1024 * 1024),
        )(left_op, left_start, right_op, right_start)
        return xl, hl, xr, hr

    op_spec = P(("batch", "row"), "col")
    vec_spec = P(("batch", "row", "col"), None)
    small_spec = P("batch", None)
    return jax.shard_map(local_program, mesh=mesh, in_specs=(op_spec, vec_spec, op_spec, vec_spec), out_specs=(vec_spec, small_spec, vec_spec, small_spec), check_vma=False)
```

```python
import jax
import jax.numpy as jnp
from jax import lax
from jax.experimental import pallas as pl
from jax.experimental.pallas import tpu as pltpu
from jax.sharding import PartitionSpec as P

SWEEPS = 4
MESH = pl.DeviceIdType.MESH
HI = lax.Precision.HIGHEST
NB = 32


def dot_hi(a, b, dims):
    return lax.dot_general(a, b, (dims, ((), ())), precision=HI, preferred_element_type=jnp.float32)


def diag_block(blk_l, blk_r, lane0):
    lane = lax.broadcasted_iota(jnp.int32, (NB, 128), 1)
    row = lax.broadcasted_iota(jnp.int32, (NB, 128), 0)
    is_left = (lane // NB) % 2 == 0
    groups = NB // 8
    cols = []
    for g in range(groups):
        r0 = 8 * g
        cols.append(jnp.stack([
            jnp.where(is_left[r0:], blk_l[r0:, lane0 + k:lane0 + k + 1], blk_r[r0:, lane0 + k:lane0 + k + 1])
            for k in range(r0, r0 + 8)]))
    w = jnp.where(lane % NB == row, 1.0, 0.0)
    piv = []
    for j in range(NB):
        g0, jj = divmod(j, 8)
        r0 = 8 * g0
        u = cols[g0][0]
        p = u[jj:jj + 1]
        piv.append(p)
        if j == NB - 1:
            break
        m = jnp.where(row[r0:] > j, u * (1.0 / p), 0.0)
        if jj < 7:
            cols[g0] = cols[g0][1:] - m[None] * u[jj + 1:8][:, None, :]
        for g in range(g0 + 1, groups):
            d = 8 * (g - g0)
            cols[g] = cols[g] - m[d:][None] * u[d:d + 8][:, None, :]
        w_low = w[r0:] - m * w[j:j + 1]
        w = w_low if g0 == 0 else jnp.concatenate([w[:r0], w_low], axis=0)
    return w * lax.rsqrt(jnp.concatenate(piv, axis=0))


def chol_inverse(s, w):
    lane64 = lax.broadcasted_iota(jnp.int32, (NB, 128), 1)
    rowi = lax.broadcasted_iota(jnp.int32, (256, 256), 0)
    lanei = lax.broadcasted_iota(jnp.int32, (256, 256), 1)
    for o in range(2):
        w[o] = jnp.where(rowi == lanei, 1.0, 0.0)
    for h in range(2):
        base = 128 * h
        for b in range(4):
            r0 = base + NB * b
            rows = slice(r0, r0 + NB)
            grp = slice(base, base + 128)
            li = diag_block(s[0, rows, grp], s[1, rows, grp], NB * b)
            lhs = jnp.concatenate([jnp.where(lane64 < NB, li, 0.0), jnp.where((lane64 >= NB) & (lane64 < 2 * NB), li, 0.0)], axis=0)[:, :2 * NB]
            rhs = jnp.concatenate([jnp.concatenate([s[o, rows, base:256], w[o, rows, 0:base + 128]], axis=1) for o in range(2)], axis=0)
            pan = dot_hi(lhs, rhs, ((1,), (0,)))
            ns = 256 - base
            for o in range(2):
                po = pan[NB * o:NB * o + NB]
                s[o, rows, base:256] = po[:, :ns]
                w[o, rows, 0:base + 128] = po[:, ns:]
                if b < 3:
                    pt = po[:, 0:128].T[NB * (b + 1):]
                    upd = dot_hi(pt, po, ((1,), (0,)))
                    rest = slice(r0 + NB, base + 128)
                    s[o, rest, base:256] = s[o, rest, base:256] - upd[:, :ns]
                    w[o, rest, 0:base + 128] = w[o, rest, 0:base + 128] - upd[:, ns:]
        if h == 0:
            for o in range(2):
                pb = s[o, 0:128, 128:256]
                full = jnp.concatenate([pb, w[o, 0:128, 0:128]], axis=1)
                upd = dot_hi(pb.T, full, ((1,), (0,)))
                s[o, 128:256, 128:256] = s[o, 128:256, 128:256] - upd[:, :128]
                w[o, 128:256, 0:128] = w[o, 128:256, 0:128] - upd[:, 128:]


def remote(src, dst, send_sem, recv_sem, row, col):
    return pltpu.make_async_remote_copy(src_ref=src, dst_ref=dst, send_sem=send_sem, recv_sem=recv_sem, device_id={"row": row, "col": col}, device_id_type=MESH)


def place():
    z = lax.axis_index("row")
    c = lax.axis_index("col")
    return z, c, c // 2, c % 2


def entry_barrier():
    z, c, y, core = place()
    barrier = pltpu.get_barrier_semaphore()
    peers = []
    k = z * 2 + y
    for e in range(1, 8):
        q = (k + e) % 8
        peers.append((q // 2, (q % 2) * 2 + core))
    peers.append((z, 2 * y + 1 - core))
    peers.append((z, 2 * (1 - y) + 1 - core))
    for row, col in peers:
        pl.semaphore_signal(barrier, inc=1, device_id={"row": row, "col": col}, device_id_type=MESH)
    pl.semaphore_wait(barrier, len(peers))


def product(ops, xs, ys, bufs):
    z, c, y, core = place()
    xb, zbuf, xcol, zs, zr, cs, cr = bufs["gather"]
    dsend, drecv, ysend, yrecv, ds, dr_sem, yss, yrs = bufs["scatter"]
    partner = 2 * y + 1 - core
    across = 2 * (1 - y) + core
    units = ((0, 0, 128), (0, 128, 256), (1, 0, 256))

    def has(way, h):
        return z >= h if way == 0 else z + h <= 3

    def onward(way, h):
        return (z >= h) & (z < 3) if way == 0 else (z + h <= 3) & (z > 0)

    def hop(u, way, h):
        src = xb[u] if h == 0 else zbuf[u].at[3 * way + h - 1]
        at = 3 * way + h
        row = (z + 1) % 4 if way == 0 else (z + 3) % 4
        return remote(src, zbuf[u].at[at], zs.at[u, at], zr.at[u, at], row, c)

    def cross(u, slot):
        src = xb[u] if slot == 6 else zbuf[u].at[slot]
        way, h = (0, 0) if slot == 6 else (slot // 3, slot % 3 + 1)
        to = (z + 4 - h) % 4 if way == 0 else (z + h) % 4
        return src, to, remote(src, xcol[u].at[c], cs.at[u, slot], cr.at[u, c], z, to)

    def start_cross(u, slot):
        src, to, copy = cross(u, slot)

        @pl.when(to != c)
        def _():
            copy.start()

        @pl.when(to == c)
        def _():
            xcol[u][c] = src[...]

    def own(u):
        o, c0, c1 = units[u]
        xb[u][...] = xs[o][:, c0:c1].astype(jnp.bfloat16)
        for way in range(2):
            @pl.when(onward(way, 0))
            def _():
                hop(u, way, 0).start()
        start_cross(u, 6)

    def arrive(u, h):
        for way in range(2):
            slot = 3 * way + h - 1

            @pl.when(has(way, h))
            def _():
                hop(u, way, h - 1).wait_recv()
                if h < 3:
                    @pl.when(onward(way, h))
                    def _():
                        hop(u, way, h).start()
                start_cross(u, slot)

    def d2d(u, i):
        return remote(dsend[u].at[i], drecv[u].at[i], ds.at[u, i], dr_sem.at[u, i], z, partner)

    def yhop(u):
        return remote(ysend[u], yrecv[u], yss.at[u], yrs.at[u], z, across)

    def compute(u):
        o, c0, c1 = units[u]
        for e in range(1, 4):
            frm = (c + e) % 4
            remote(xb[u], xcol[u].at[frm], cs.at[u, 6], cr.at[u, frm], z, frm).wait_recv()
        n = xs[o].shape[0]
        full = xcol[u][...].reshape(4 * n, c1 - c0)

        def part(q):
            return jnp.dot(ops[o][pl.ds(pl.multiple_of(q * n, n), n), :], full, preferred_element_type=jnp.float32)

        dsend[u][0] = part(2 * (1 - y) + 1 - core)
        d2d(u, 0).start()
        far = part(2 * (1 - y) + core)
        dsend[u][1] = part(2 * y + 1 - core)
        d2d(u, 1).start()
        d2d(u, 0).wait_recv()
        ysend[u][...] = far + drecv[u][0]
        yhop(u).start()
        near = part(2 * y + core)
        d2d(u, 1).wait_recv()
        ys[o][:, c0:c1] = near + drecv[u][1]

    own(0)
    own(1)
    arrive(0, 1)
    own(2)
    arrive(1, 1)
    arrive(0, 2)
    arrive(2, 1)
    arrive(1, 2)
    arrive(0, 3)
    arrive(2, 2)
    arrive(1, 3)
    compute(0)
    arrive(2, 3)
    compute(1)
    compute(2)
    for u, (o, c0, c1) in enumerate(units):
        yhop(u).wait_recv()
        ys[o][:, c0:c1] = ys[o][:, c0:c1] + yrecv[u][...]
    for u in range(3):
        yhop(u).wait_send()
        for i in range(2):
            d2d(u, i).wait_send()
        for way in range(2):
            for h in range(3):
                @pl.when(onward(way, h))
                def _():
                    hop(u, way, h).wait_send()
        for slot in range(7):
            _, to, copy = cross(u, slot)
            here = True if slot == 6 else has(slot // 3, slot % 3 + 1)

            @pl.when((to != c) & here)
            def _():
                copy.wait_send()


def all_sum(half, bufs):
    z, c, y, core = place()
    gp, r1, acc, r2, res, s1, s2, s3, s4, v1, v2, v3, v4 = bufs["sum"]
    partner = 2 * y + 1 - core
    piece = half // 8
    k = z * 2 + y

    def peer(e):
        q = (k + e) % 8
        return q, q // 2, (q % 2) * 2 + core

    one = remote(gp.at[1 - core, pl.ds(0, half)], r1.at[pl.ds(0, half)], s1, v1, z, partner)
    one.start()
    one.wait_recv()
    acc[0:half] = gp[core, 0:half] + r1[0:half]

    def spread(e):
        q, row, col = peer(e)
        return remote(acc.at[pl.ds(pl.multiple_of(q * piece, piece), piece)], r2.at[e, pl.ds(0, piece)], s2.at[e], v2.at[e], row, col)

    order = (4, 3, 5, 2, 6, 1, 7)
    for e in order:
        spread(e).start()
    mine = pl.ds(pl.multiple_of(k * piece, piece), piece)
    total = acc[mine]
    for e in range(1, 8):
        spread(e).wait_recv()
        total = total + r2[e, 0:piece]
    res[core, mine] = total

    def share(e, slot):
        q, row, col = peer(e)
        at = pl.ds(pl.multiple_of(slot * piece, piece), piece)
        return remote(res.at[core, at], res.at[core, at], s3.at[e], v3.at[e], row, col)

    for e in order:
        share(e, k).start()
    for e in range(1, 8):
        share(e, (k + 8 - e) % 8).wait_recv()
    last = remote(res.at[core, pl.ds(0, half)], res.at[core, pl.ds(0, half)], s4, v4, z, partner)
    last.start()
    got = remote(res.at[1 - core, pl.ds(0, half)], res.at[1 - core, pl.ds(0, half)], s4, v4, z, partner)
    got.wait_recv()
    one.wait_send()
    for e in range(1, 8):
        spread(e).wait_send()
        share(e, k).wait_send()
    last.wait_send()


def pack_gram(mats, precision, gp):
    for o in range(2):
        g = lax.dot_general(mats[o], mats[o], (((0,), (0,)), ((), ())), precision=precision, preferred_element_type=jnp.float32)
        gp[o, 0:128] = g[0:128, 0:128]
        gp[o, 128:256] = g[0:128, 128:256]
        gp[o, 256:384] = g[128:256, 128:256]


def body(lop, lx, rop, rx, xl_out, hl_out, xr_out, hr_out, lv, rv, xl, xr, yl, yr, s, w, *rest):
    names = iter(rest)

    def take(n):
        return [next(names) for _ in range(n)]

    xb, zbuf, xcol = take(3), take(3), take(3)
    gsems = take(4)
    dsend, drecv, ysend, yrecv = take(3), take(3), take(3), take(3)
    ssems = take(4)
    bufs = {"gather": (xb, zbuf, xcol, *gsems), "scatter": (dsend, drecv, ysend, yrecv, *ssems), "sum": take(13)}
    (lsem,) = take(1)
    loads = [pltpu.make_async_copy(lop, lv, lsem.at[0]), pltpu.make_async_copy(rop, rv, lsem.at[1])]
    for load in loads:
        load.start()
    xs, ys, ops = (xl, xr), (yl, yr), (lv, rv)
    scales = [1.0 / (16 * ref.shape[0]) for ref in xs]
    xl[...] = lx[...]
    xr[...] = rx[...]
    entry_barrier()
    for load in loads:
        load.wait()

    gp, res = bufs["sum"][0], bufs["sum"][4]

    def half_step(phase, carry):
        @pl.when(phase == 0)
        def _():
            pack_gram([r[...].astype(jnp.bfloat16) for r in ys], None, gp)

        @pl.when(phase == 1)
        def _():
            pack_gram([r[...] for r in ys], HI, gp)

        all_sum(384, bufs)
        for o in range(2):
            s[o, 0:128, 0:128] = res[o, 0:128] * scales[o]
            s[o, 0:128, 128:256] = res[o, 128:256] * scales[o]
            s[o, 128:256, 128:256] = res[o, 256:384] * scales[o]
        chol_inverse(s, w)
        for o in range(2):
            ys[o][...] = dot_hi(ys[o][...], w[o], ((1,), (1,)))
        return carry

    def sweep(i, carry):
        product(ops, xs, ys, bufs)
        lax.fori_loop(0, 2, half_step, 0)
        for o in range(2):
            xs[o][...] = ys[o][...]
        return carry

    lax.fori_loop(0, SWEEPS, sweep, 0)
    product(ops, xs, ys, bufs)
    for o in range(2):
        h = dot_hi(xs[o][...], ys[o][...], ((0,), (0,)))
        gp[o, 0:256] = h[:, 0:128]
        gp[o, 256:512] = h[:, 128:256]
    all_sum(512, bufs)
    for o, out in enumerate((hl_out, hr_out)):
        out[:, 0:128] = res[o, 0:256] * scales[o]
        out[:, 128:256] = res[o, 256:512] * scales[o]
    xl_out[...] = xl[...]
    xr_out[...] = xr[...]


def solution(mesh):
    f32, bf16 = jnp.float32, jnp.bfloat16

    def local_program(left_op, left_start, right_op, right_start):
        nl, nr = left_start.shape[0], right_start.shape[0]
        vm = pl.BlockSpec(memory_space=pltpu.VMEM)
        hbm = pl.BlockSpec(memory_space=pl.ANY)
        dma = pltpu.SemaphoreType.DMA

        def pair(shape, dtype):
            return [pltpu.VMEM(shape(nl), dtype), pltpu.VMEM(shape(nr), dtype)]

        def units(lead, dtype):
            return [pltpu.VMEM(lead + tail, dtype) for tail in ((nl, 128), (nl, 128), (nr, 256))]

        scratch = [pltpu.VMEM(left_op.shape, bf16), pltpu.VMEM(right_op.shape, bf16)]
        scratch += pair(lambda n: (n, 256), f32) + pair(lambda n: (n, 256), f32)
        scratch += [pltpu.VMEM((2, 256, 256), f32), pltpu.VMEM((2, 256, 256), f32)]
        for lead in ((), (6,), (4,)):
            scratch += units(lead, bf16)
        scratch += [dma((3, 6)), dma((3, 6)), dma((3, 7)), dma((3, 4))]
        for lead in ((2,), (2,), (), ()):
            scratch += units(lead, f32)
        scratch += [dma((3, 2)), dma((3, 2)), dma((3,)), dma((3,))]
        scratch += [pltpu.VMEM((2, 512, 128), f32), pltpu.VMEM((512, 128), f32), pltpu.VMEM((512, 128), f32), pltpu.VMEM((8, 64, 128), f32), pltpu.VMEM((2, 512, 128), f32)]
        scratch += [dma, dma((8,)), dma((8,)), dma, dma, dma((8,)), dma((8,)), dma]
        scratch += [dma((2,))]
        small = jax.ShapeDtypeStruct((256, 256), f32)
        xl, hl, xr, hr = pl.pallas_call(
            body,
            out_shape=(jax.ShapeDtypeStruct((nl, 256), f32), small, jax.ShapeDtypeStruct((nr, 256), f32), small),
            in_specs=[hbm, vm, hbm, vm],
            out_specs=(vm, vm, vm, vm),
            scratch_shapes=scratch,
            compiler_params=pltpu.CompilerParams(collective_id=0, has_side_effects=True, vmem_limit_bytes=60 * 1024 * 1024),
        )(left_op, left_start, right_op, right_start)
        return xl, hl, xr, hr

    op_spec = P(("batch", "row"), "col")
    vec_spec = P(("batch", "row", "col"), None)
    small_spec = P("batch", None)
    return jax.shard_map(local_program, mesh=mesh, in_specs=(op_spec, vec_spec, op_spec, vec_spec), out_specs=(vec_spec, small_spec, vec_spec, small_spec), check_vma=False)
```

```python
import jax
import jax.numpy as jnp
from jax import lax
from jax.experimental import pallas as pl
from jax.experimental.pallas import tpu as pltpu
from jax.sharding import PartitionSpec as P

SWEEPS = 4
MESH = pl.DeviceIdType.MESH
HI = lax.Precision.HIGHEST
NB = 32


def dot_hi(a, b, dims):
    return lax.dot_general(a, b, (dims, ((), ())), precision=HI, preferred_element_type=jnp.float32)


def diag_block(blk_l, blk_r, lane0):
    lane = lax.broadcasted_iota(jnp.int32, (NB, 128), 1)
    row = lax.broadcasted_iota(jnp.int32, (NB, 128), 0)
    is_left = (lane // NB) % 2 == 0
    groups = NB // 8
    cols = []
    for g in range(groups):
        r0 = 8 * g
        cols.append(jnp.stack([
            jnp.where(is_left[r0:], blk_l[r0:, lane0 + k:lane0 + k + 1], blk_r[r0:, lane0 + k:lane0 + k + 1])
            for k in range(r0, r0 + 8)]))
    w = jnp.where(lane % NB == row, 1.0, 0.0)
    piv = []
    for j in range(NB):
        g0, jj = divmod(j, 8)
        r0 = 8 * g0
        u = cols[g0][0]
        p = u[jj:jj + 1]
        piv.append(p)
        if j == NB - 1:
            break
        m = jnp.where(row[r0:] > j, u * (1.0 / p), 0.0)
        if jj < 7:
            cols[g0] = cols[g0][1:] - m[None] * u[jj + 1:8][:, None, :]
        for g in range(g0 + 1, groups):
            d = 8 * (g - g0)
            cols[g] = cols[g] - m[d:][None] * u[d:d + 8][:, None, :]
        w_low = w[r0:] - m * w[j:j + 1]
        w = w_low if g0 == 0 else jnp.concatenate([w[:r0], w_low], axis=0)
    return w * lax.rsqrt(jnp.concatenate(piv, axis=0))


def chol_inverse(s, w):
    lane64 = lax.broadcasted_iota(jnp.int32, (NB, 128), 1)
    rowi = lax.broadcasted_iota(jnp.int32, (256, 256), 0)
    lanei = lax.broadcasted_iota(jnp.int32, (256, 256), 1)
    for o in range(2):
        w[o] = jnp.where(rowi == lanei, 1.0, 0.0)
    for h in range(2):
        base = 128 * h
        for b in range(4):
            r0 = base + NB * b
            rows = slice(r0, r0 + NB)
            grp = slice(base, base + 128)
            li = diag_block(s[0, rows, grp], s[1, rows, grp], NB * b)
            lhs = jnp.concatenate([jnp.where(lane64 < NB, li, 0.0), jnp.where((lane64 >= NB) & (lane64 < 2 * NB), li, 0.0)], axis=0)[:, :2 * NB]
            rhs = jnp.concatenate([jnp.concatenate([s[o, rows, base:256], w[o, rows, 0:base + 128]], axis=1) for o in range(2)], axis=0)
            pan = dot_hi(lhs, rhs, ((1,), (0,)))
            ns = 256 - base
            for o in range(2):
                po = pan[NB * o:NB * o + NB]
                s[o, rows, base:256] = po[:, :ns]
                w[o, rows, 0:base + 128] = po[:, ns:]
                if b < 3:
                    pt = po[:, 0:128].T[NB * (b + 1):]
                    upd = dot_hi(pt, po, ((1,), (0,)))
                    rest = slice(r0 + NB, base + 128)
                    s[o, rest, base:256] = s[o, rest, base:256] - upd[:, :ns]
                    w[o, rest, 0:base + 128] = w[o, rest, 0:base + 128] - upd[:, ns:]
        if h == 0:
            for o in range(2):
                pb = s[o, 0:128, 128:256]
                full = jnp.concatenate([pb, w[o, 0:128, 0:128]], axis=1)
                upd = dot_hi(pb.T, full, ((1,), (0,)))
                s[o, 128:256, 128:256] = s[o, 128:256, 128:256] - upd[:, :128]
                w[o, 128:256, 0:128] = w[o, 128:256, 0:128] - upd[:, 128:]


def remote(src, dst, send_sem, recv_sem, row, col):
    return pltpu.make_async_remote_copy(src_ref=src, dst_ref=dst, send_sem=send_sem, recv_sem=recv_sem, device_id={"row": row, "col": col}, device_id_type=MESH)


def place():
    z = lax.axis_index("row")
    c = lax.axis_index("col")
    return z, c, c // 2, c % 2


def entry_barrier():
    z, c, y, core = place()
    barrier = pltpu.get_barrier_semaphore()
    peers = []
    k = z * 2 + y
    for e in range(1, 8):
        q = (k + e) % 8
        peers.append((q // 2, (q % 2) * 2 + core))
    peers.append((z, 2 * y + 1 - core))
    peers.append((z, 2 * (1 - y) + 1 - core))
    for row, col in peers:
        pl.semaphore_signal(barrier, inc=1, device_id={"row": row, "col": col}, device_id_type=MESH)
    pl.semaphore_wait(barrier, len(peers))


def product(ops, xs, ys, bufs):
    z, c, y, core = place()
    xb, obuf, xcol, ss, rr, orr = bufs["gather"]
    dsend, drecv, ysend, yrecv, ds, dr_sem, yss, yrs = bufs["scatter"]
    partner = 2 * y + 1 - core
    across = 2 * (1 - y) + core
    units = ((1, 0, 256), (0, 0, 128), (0, 128, 256))
    t = z + y * (3 - 2 * z)
    kind = core + y * (1 - 2 * core)
    home = t == kind
    step = 1 - 2 * y
    ahead, back = (z + step + 4) % 4, (z - step + 4) % 4
    slots = (c, partner, 2 * (1 - y), 2 * (1 - y) + 1)
    inner = jnp.where(t == 3, 0, 1)
    target = 2 * (1 - y) + jnp.where(y == 1, inner, 1 - inner)

    def goes_ahead(i):
        return ((kind == 0) & (t < 3)) | ((kind == 1) & (t >= 1) & (t < 3) & (i < 2))

    goes_back = (kind == 1) & (t == 1)

    def pass_on(u, i, way):
        at = xcol[u].at[slots[i]]
        return remote(at, at, ss.at[u, 4 * way + i], rr.at[u, slots[i]], back if way else ahead, c)

    def start_passes(u, i):
        @pl.when(goes_ahead(i))
        def _():
            pass_on(u, i, 0).start()

        @pl.when(goes_back)
        def _():
            pass_on(u, i, 1).start()

    def to_partner(u):
        return remote(xb[u], xcol[u].at[c], ss.at[u, 8], rr.at[u, c], z, partner)

    gives = (t == 1 - kind) & (t < 2)

    def cross(u, src):
        return remote(src, xcol[u].at[c], ss.at[u, 9], rr.at[u, c], z, target)

    def ride(u, src):
        return remote(src, obuf[u], ss.at[u, 10], orr.at[u], back, c)

    def arrived(u, i):
        remote(xb[u], xcol[u].at[slots[i]], ss.at[u, 9], rr.at[u, slots[i]], z, target).wait_recv()

    def own(u):
        o, c0, c1 = units[u]
        xb[u][...] = xs[o][:, c0:c1].astype(jnp.bfloat16)

        @pl.when(t >= 2)
        def _():
            cross(u, xb[u]).start()

        @pl.when(t == 2)
        def _():
            ride(u, xb[u]).start()

        @pl.when(gives)
        def _():
            to_partner(u).start()

        @pl.when(home)
        def _():
            xcol[u][c] = xb[u][...]
            start_passes(u, 0)

    def stage(u, i, who=True):
        @pl.when((goes_ahead(i) | goes_back) & who)
        def _():
            if i == 0:
                @pl.when(jnp.logical_not(home))
                def _():
                    arrived(u, 0)
                    start_passes(u, 0)
            else:
                arrived(u, i)
                start_passes(u, i)

    def transit(u, at):
        @pl.when(t == at)
        def _():
            ride(u, xb[u]).wait_recv()
            if at == 1:
                ride(u, obuf[u]).start()
            cross(u, obuf[u]).start()

    def d2d(u, i):
        return remote(dsend[u].at[i, 1 - core], drecv[u].at[i], ds.at[u, i], dr_sem.at[u, i], z, partner)

    def yhop(u):
        return remote(ysend[u], yrecv[u], yss.at[u], yrs.at[u], z, across)

    def compute(u):
        o, c0, c1 = units[u]
        for i in range(4):
            @pl.when(jnp.logical_not(goes_ahead(i) | goes_back))
            def _():
                arrived(u, i)

        n = xs[o].shape[0]
        full = xcol[u][...].reshape(4 * n, c1 - c0)

        def half_rows(i, of):
            rows = ops[o][pl.ds(pl.multiple_of(of * 2 * n, 2 * n), 2 * n), :]
            dsend[u][i] = jnp.dot(rows, full, preferred_element_type=jnp.float32).reshape(2, n, c1 - c0)
            d2d(u, i).start()

        half_rows(0, 1 - y)
        half_rows(1, y)
        d2d(u, 0).wait_recv()
        ysend[u][...] = dsend[u][0, core] + drecv[u][0]
        yhop(u).start()
        d2d(u, 1).wait_recv()
        ys[o][:, c0:c1] = dsend[u][1, core] + drecv[u][1]

    own(0)
    own(1)
    stage(0, 0)
    stage(0, 1)
    own(2)
    transit(0, 1)
    stage(0, 2)
    stage(0, 3)
    stage(1, 0)
    stage(1, 1)
    transit(1, 1)
    stage(1, 2)
    stage(1, 3)
    for i in range(4):
        stage(2, i, t == 0)
    transit(0, 0)
    transit(1, 0)
    compute(0)
    stage(2, 0, t > 0)
    stage(2, 1, t > 0)
    transit(2, 1)
    stage(2, 2, t > 0)
    stage(2, 3, t > 0)
    transit(2, 0)
    compute(1)
    compute(2)
    for u, (o, c0, c1) in enumerate(units):
        yhop(u).wait_recv()
        ys[o][:, c0:c1] = ys[o][:, c0:c1] + yrecv[u][...]
    for u in range(3):
        yhop(u).wait_send()
        for i in range(2):
            d2d(u, i).wait_send()
        for i in range(4):
            @pl.when(goes_ahead(i))
            def _():
                pass_on(u, i, 0).wait_send()

            @pl.when(goes_back)
            def _():
                pass_on(u, i, 1).wait_send()

        @pl.when(gives)
        def _():
            to_partner(u).wait_send()

        cross(u, xb[u]).wait_send()

        @pl.when((t == 1) | (t == 2))
        def _():
            ride(u, xb[u]).wait_send()


def all_sum(half, bufs):
    z, c, y, core = place()
    gp, r1, acc, r2, res, s1, s2, s3, s4, v1, v2, v3, v4 = bufs["sum"]
    partner = 2 * y + 1 - core
    piece = half // 8
    k = z * 2 + y

    def peer(e):
        q = (k + e) % 8
        return q, q // 2, (q % 2) * 2 + core

    one = remote(gp.at[1 - core, pl.ds(0, half)], r1.at[pl.ds(0, half)], s1, v1, z, partner)
    one.start()
    one.wait_recv()
    acc[0:half] = gp[core, 0:half] + r1[0:half]

    def spread(e):
        q, row, col = peer(e)
        return remote(acc.at[pl.ds(pl.multiple_of(q * piece, piece), piece)], r2.at[e, pl.ds(0, piece)], s2.at[e], v2.at[e], row, col)

    order = (4, 3, 5, 2, 6, 1, 7)
    for e in order:
        spread(e).start()
    mine = pl.ds(pl.multiple_of(k * piece, piece), piece)
    total = acc[mine]
    for e in range(1, 8):
        spread(e).wait_recv()
        total = total + r2[e, 0:piece]
    res[core, mine] = total

    def share(e, slot):
        q, row, col = peer(e)
        at = pl.ds(pl.multiple_of(slot * piece, piece), piece)
        return remote(res.at[core, at], res.at[core, at], s3.at[e], v3.at[e], row, col)

    for e in order:
        share(e, k).start()
    for e in range(1, 8):
        share(e, (k + 8 - e) % 8).wait_recv()
    last = remote(res.at[core, pl.ds(0, half)], res.at[core, pl.ds(0, half)], s4, v4, z, partner)
    last.start()
    got = remote(res.at[1 - core, pl.ds(0, half)], res.at[1 - core, pl.ds(0, half)], s4, v4, z, partner)
    got.wait_recv()
    one.wait_send()
    for e in range(1, 8):
        spread(e).wait_send()
        share(e, k).wait_send()
    last.wait_send()


def pack_gram(mats, precision, gp):
    for o in range(2):
        g = lax.dot_general(mats[o], mats[o], (((0,), (0,)), ((), ())), precision=precision, preferred_element_type=jnp.float32)
        gp[o, 0:128] = g[0:128, 0:128]
        gp[o, 128:256] = g[0:128, 128:256]
        gp[o, 256:384] = g[128:256, 128:256]


def body(lop, lx, rop, rx, xl_out, hl_out, xr_out, hr_out, lv, rv, xl, xr, yl, yr, s, w, *rest):
    names = iter(rest)

    def take(n):
        return [next(names) for _ in range(n)]

    xb, obuf, xcol = take(3), take(3), take(3)
    gsems = take(3)
    dsend, drecv, ysend, yrecv = take(3), take(3), take(3), take(3)
    ssems = take(4)
    bufs = {"gather": (xb, obuf, xcol, *gsems), "scatter": (dsend, drecv, ysend, yrecv, *ssems), "sum": take(13)}
    (lsem,) = take(1)
    loads = [pltpu.make_async_copy(lop, lv, lsem.at[0]), pltpu.make_async_copy(rop, rv, lsem.at[1])]
    for load in loads:
        load.start()
    xs, ys, ops = (xl, xr), (yl, yr), (lv, rv)
    scales = [1.0 / (16 * ref.shape[0]) for ref in xs]
    xl[...] = lx[...]
    xr[...] = rx[...]
    entry_barrier()
    for load in loads:
        load.wait()

    gp, res = bufs["sum"][0], bufs["sum"][4]

    def half_step(phase, carry):
        @pl.when(phase == 0)
        def _():
            pack_gram([r[...].astype(jnp.bfloat16) for r in ys], None, gp)

        @pl.when(phase == 1)
        def _():
            pack_gram([r[...] for r in ys], HI, gp)

        all_sum(384, bufs)
        for o in range(2):
            s[o, 0:128, 0:128] = res[o, 0:128] * scales[o]
            s[o, 0:128, 128:256] = res[o, 128:256] * scales[o]
            s[o, 128:256, 128:256] = res[o, 256:384] * scales[o]
        chol_inverse(s, w)
        for o in range(2):
            ys[o][...] = dot_hi(ys[o][...], w[o], ((1,), (1,)))
        return carry

    def sweep(i, carry):
        product(ops, xs, ys, bufs)
        lax.fori_loop(0, 2, half_step, 0)
        for o in range(2):
            xs[o][...] = ys[o][...]
        return carry

    lax.fori_loop(0, SWEEPS, sweep, 0)
    product(ops, xs, ys, bufs)
    for o in range(2):
        h = dot_hi(xs[o][...], ys[o][...], ((0,), (0,)))
        gp[o, 0:256] = h[:, 0:128]
        gp[o, 256:512] = h[:, 128:256]
    all_sum(512, bufs)
    for o, out in enumerate((hl_out, hr_out)):
        out[:, 0:128] = res[o, 0:256] * scales[o]
        out[:, 128:256] = res[o, 256:512] * scales[o]
    xl_out[...] = xl[...]
    xr_out[...] = xr[...]


def solution(mesh):
    f32, bf16 = jnp.float32, jnp.bfloat16

    def local_program(left_op, left_start, right_op, right_start):
        nl, nr = left_start.shape[0], right_start.shape[0]
        vm = pl.BlockSpec(memory_space=pltpu.VMEM)
        hbm = pl.BlockSpec(memory_space=pl.ANY)
        dma = pltpu.SemaphoreType.DMA

        def pair(shape, dtype):
            return [pltpu.VMEM(shape(nl), dtype), pltpu.VMEM(shape(nr), dtype)]

        def units(lead, dtype):
            return [pltpu.VMEM(lead + tail, dtype) for tail in ((nr, 256), (nl, 128), (nl, 128))]

        scratch = [pltpu.VMEM(left_op.shape, bf16), pltpu.VMEM(right_op.shape, bf16)]
        scratch += pair(lambda n: (n, 256), f32) + pair(lambda n: (n, 256), f32)
        scratch += [pltpu.VMEM((2, 256, 256), f32), pltpu.VMEM((2, 256, 256), f32)]
        for lead in ((), (), (4,)):
            scratch += units(lead, bf16)
        scratch += [dma((3, 11)), dma((3, 4)), dma((3,))]
        for lead in ((2, 2), (2,), (), ()):
            scratch += units(lead, f32)
        scratch += [dma((3, 2)), dma((3, 2)), dma((3,)), dma((3,))]
        scratch += [pltpu.VMEM((2, 512, 128), f32), pltpu.VMEM((512, 128), f32), pltpu.VMEM((512, 128), f32), pltpu.VMEM((8, 64, 128), f32), pltpu.VMEM((2, 512, 128), f32)]
        scratch += [dma, dma((8,)), dma((8,)), dma, dma, dma((8,)), dma((8,)), dma]
        scratch += [dma((2,))]
        small = jax.ShapeDtypeStruct((256, 256), f32)
        xl, hl, xr, hr = pl.pallas_call(
            body,
            out_shape=(jax.ShapeDtypeStruct((nl, 256), f32), small, jax.ShapeDtypeStruct((nr, 256), f32), small),
            in_specs=[hbm, vm, hbm, vm],
            out_specs=(vm, vm, vm, vm),
            scratch_shapes=scratch,
            compiler_params=pltpu.CompilerParams(collective_id=0, has_side_effects=True, vmem_limit_bytes=60 * 1024 * 1024),
        )(left_op, left_start, right_op, right_start)
        return xl, hl, xr, hr

    op_spec = P(("batch", "row"), "col")
    vec_spec = P(("batch", "row", "col"), None)
    small_spec = P("batch", None)
    return jax.shard_map(local_program, mesh=mesh, in_specs=(op_spec, vec_spec, op_spec, vec_spec), out_specs=(vec_spec, small_spec, vec_spec, small_spec), check_vma=False)
```

```python
import jax
import jax.numpy as jnp
from jax import lax
from jax.experimental import pallas as pl
from jax.experimental.pallas import tpu as pltpu
from jax.sharding import PartitionSpec as P

SWEEPS = 4
MESH = pl.DeviceIdType.MESH
HI = lax.Precision.HIGHEST
NB = 32


def dot_hi(a, b, dims):
    return lax.dot_general(a, b, (dims, ((), ())), precision=HI, preferred_element_type=jnp.float32)


def diag_block(blk, lane0):
    lane = lax.broadcasted_iota(jnp.int32, (NB, 128), 1)
    row = lax.broadcasted_iota(jnp.int32, (NB, 128), 0)
    groups = NB // 8
    cols = []
    for g in range(groups):
        r0 = 8 * g
        cols.append(jnp.stack([
            jnp.broadcast_to(blk[r0:, lane0 + k:lane0 + k + 1], (NB - r0, 128)) for k in range(r0, r0 + 8)]))
    w = jnp.where(lane % NB == row, 1.0, 0.0)
    piv = []
    for j in range(NB):
        g0, jj = divmod(j, 8)
        r0 = 8 * g0
        u = cols[g0][0]
        p = u[jj:jj + 1]
        piv.append(p)
        if j == NB - 1:
            break
        m = jnp.where(row[r0:] > j, u * (1.0 / p), 0.0)
        if jj < 7:
            cols[g0] = cols[g0][1:] - m[None] * u[jj + 1:8][:, None, :]
        for g in range(g0 + 1, groups):
            d = 8 * (g - g0)
            cols[g] = cols[g] - m[d:][None] * u[d:d + 8][:, None, :]
        w_low = w[r0:] - m * w[j:j + 1]
        w = w_low if g0 == 0 else jnp.concatenate([w[:r0], w_low], axis=0)
    return w * lax.rsqrt(jnp.concatenate(piv, axis=0))


def chol_inverse(s, w):
    rowi = lax.broadcasted_iota(jnp.int32, (256, 256), 0)
    lanei = lax.broadcasted_iota(jnp.int32, (256, 256), 1)
    w[...] = jnp.where(rowi == lanei, 1.0, 0.0)
    for h in range(2):
        base = 128 * h
        for b in range(4):
            r0 = base + NB * b
            rows = slice(r0, r0 + NB)
            li = diag_block(s[rows, base:base + 128], NB * b)
            pan = dot_hi(li[:, :NB], jnp.concatenate([s[rows, base:256], w[rows, 0:base + 128]], axis=1), ((1,), (0,)))
            ns = 256 - base
            s[rows, base:256] = pan[:, :ns]
            w[rows, 0:base + 128] = pan[:, ns:]
            if b < 3:
                upd = dot_hi(pan[:, 0:128].T[NB * (b + 1):], pan, ((1,), (0,)))
                rest = slice(r0 + NB, base + 128)
                s[rest, base:256] = s[rest, base:256] - upd[:, :ns]
                w[rest, 0:base + 128] = w[rest, 0:base + 128] - upd[:, ns:]
        if h == 0:
            pb = s[0:128, 128:256]
            upd = dot_hi(pb.T, jnp.concatenate([pb, w[0:128, 0:128]], axis=1), ((1,), (0,)))
            s[128:256, 128:256] = s[128:256, 128:256] - upd[:, :128]
            w[128:256, 0:128] = w[128:256, 0:128] - upd[:, 128:]


def remote(src, dst, send_sem, recv_sem, row, col):
    return pltpu.make_async_remote_copy(src_ref=src, dst_ref=dst, send_sem=send_sem, recv_sem=recv_sem, device_id={"row": row, "col": col}, device_id_type=MESH)


def place():
    z = lax.axis_index("row")
    c = lax.axis_index("col")
    return z, c, c // 2, c % 2


def entry_barrier():
    z, c, y, core = place()
    barrier = pltpu.get_barrier_semaphore()
    peers = []
    k = z * 2 + y
    for e in range(1, 8):
        q = (k + e) % 8
        peers.append((q // 2, (q % 2) * 2 + core))
    peers.append((z, 2 * y + 1 - core))
    peers.append((z, 2 * (1 - y) + 1 - core))
    for row, col in peers:
        pl.semaphore_signal(barrier, inc=1, device_id={"row": row, "col": col}, device_id_type=MESH)
    pl.semaphore_wait(barrier, len(peers))


def product(ops, xs, ys, bufs):
    z, c, y, core = place()
    xb, obuf, xcol, ss, rr, orr = bufs["gather"]
    dsend, drecv, ysend, yrecv, ds, dr_sem, yss, yrs = bufs["scatter"]
    partner = 2 * y + 1 - core
    across = 2 * (1 - y) + core
    units = ((1, 0, 256), (0, 0, 128), (0, 128, 256))
    t = z + y * (3 - 2 * z)
    kind = core + y * (1 - 2 * core)
    home = t == kind
    step = 1 - 2 * y
    ahead, back = (z + step + 4) % 4, (z - step + 4) % 4
    slots = (c, partner, 2 * (1 - y), 2 * (1 - y) + 1)
    inner = jnp.where(t == 3, 0, 1)
    target = 2 * (1 - y) + jnp.where(y == 1, inner, 1 - inner)

    def goes_ahead(i):
        return ((kind == 0) & (t < 3)) | ((kind == 1) & (t >= 1) & (t < 3) & (i < 2))

    goes_back = (kind == 1) & (t == 1)

    def pass_on(u, i, way):
        at = xcol[u].at[slots[i]]
        return remote(at, at, ss.at[u, 4 * way + i], rr.at[u, slots[i]], back if way else ahead, c)

    def start_passes(u, i):
        @pl.when(goes_ahead(i))
        def _():
            pass_on(u, i, 0).start()

        @pl.when(goes_back)
        def _():
            pass_on(u, i, 1).start()

    def to_partner(u):
        return remote(xb[u], xcol[u].at[c], ss.at[u, 8], rr.at[u, c], z, partner)

    gives = (t == 1 - kind) & (t < 2)

    def cross(u, src):
        return remote(src, xcol[u].at[c], ss.at[u, 9], rr.at[u, c], z, target)

    def ride(u, src):
        return remote(src, obuf[u], ss.at[u, 10], orr.at[u], back, c)

    def arrived(u, i):
        remote(xb[u], xcol[u].at[slots[i]], ss.at[u, 9], rr.at[u, slots[i]], z, target).wait_recv()

    def own(u):
        o, c0, c1 = units[u]
        xb[u][...] = xs[o][:, c0:c1].astype(jnp.bfloat16)

        @pl.when(t >= 2)
        def _():
            cross(u, xb[u]).start()

        @pl.when(t == 2)
        def _():
            ride(u, xb[u]).start()

        @pl.when(gives)
        def _():
            to_partner(u).start()

        @pl.when(home)
        def _():
            xcol[u][c] = xb[u][...]
            start_passes(u, 0)

    def stage(u, i, who=True):
        @pl.when((goes_ahead(i) | goes_back) & who)
        def _():
            if i == 0:
                @pl.when(jnp.logical_not(home))
                def _():
                    arrived(u, 0)
                    start_passes(u, 0)
            else:
                arrived(u, i)
                start_passes(u, i)

    def transit(u, at):
        @pl.when(t == at)
        def _():
            ride(u, xb[u]).wait_recv()
            if at == 1:
                ride(u, obuf[u]).start()
            cross(u, obuf[u]).start()

    def d2d(u, i):
        return remote(dsend[u].at[i, 1 - core], drecv[u].at[i], ds.at[u, i], dr_sem.at[u, i], z, partner)

    def yhop(u):
        return remote(ysend[u], yrecv[u], yss.at[u], yrs.at[u], z, across)

    def compute(u):
        o, c0, c1 = units[u]
        for i in range(4):
            @pl.when(jnp.logical_not(goes_ahead(i) | goes_back))
            def _():
                arrived(u, i)

        n = xs[o].shape[0]
        def half_rows(i, of):
            rows = ops[o][pl.ds(pl.multiple_of(of * 2 * n, 2 * n), 2 * n), :]
            full = xcol[u][...].reshape(4 * n, c1 - c0)
            dsend[u][i] = jnp.dot(rows, full, preferred_element_type=jnp.float32).reshape(2, n, c1 - c0)
            d2d(u, i).start()

        half_rows(0, 1 - y)
        half_rows(1, y)
        d2d(u, 0).wait_recv()
        ysend[u][...] = dsend[u][0, core] + drecv[u][0]
        yhop(u).start()
        d2d(u, 1).wait_recv()
        ys[o][:, c0:c1] = dsend[u][1, core] + drecv[u][1]

    own(0)
    own(1)
    stage(0, 0)
    stage(0, 1)
    own(2)
    transit(0, 1)
    stage(0, 2)
    stage(0, 3)
    stage(1, 0)
    stage(1, 1)
    transit(1, 1)
    stage(1, 2)
    stage(1, 3)
    for i in range(4):
        stage(2, i, t == 0)
    transit(0, 0)
    transit(1, 0)
    compute(0)
    stage(2, 0, t > 0)
    stage(2, 1, t > 0)
    transit(2, 1)
    stage(2, 2, t > 0)
    stage(2, 3, t > 0)
    transit(2, 0)
    compute(1)
    compute(2)
    for u, (o, c0, c1) in enumerate(units):
        yhop(u).wait_recv()
        ys[o][:, c0:c1] = ys[o][:, c0:c1] + yrecv[u][...]
    for u in range(3):
        yhop(u).wait_send()
        for i in range(2):
            d2d(u, i).wait_send()
        for i in range(4):
            @pl.when(goes_ahead(i))
            def _():
                pass_on(u, i, 0).wait_send()

            @pl.when(goes_back)
            def _():
                pass_on(u, i, 1).wait_send()

        @pl.when(gives)
        def _():
            to_partner(u).wait_send()

        cross(u, xb[u]).wait_send()

        @pl.when((t == 1) | (t == 2))
        def _():
            ride(u, xb[u]).wait_send()


def all_sum(half, bufs, both):
    z, c, y, core = place()
    gp, r1, acc, r2, res, s1, s2, s3, s4, v1, v2, v3, v4 = bufs["sum"]
    partner = 2 * y + 1 - core
    piece = half // 8
    k = z * 2 + y

    def peer(e):
        q = (k + e) % 8
        return q, q // 2, (q % 2) * 2 + core

    one = remote(gp.at[1 - core, pl.ds(0, half)], r1.at[pl.ds(0, half)], s1, v1, z, partner)
    one.start()
    one.wait_recv()
    acc[0:half] = gp[core, 0:half] + r1[0:half]

    def spread(e):
        q, row, col = peer(e)
        return remote(acc.at[pl.ds(pl.multiple_of(q * piece, piece), piece)], r2.at[e, pl.ds(0, piece)], s2.at[e], v2.at[e], row, col)

    order = (4, 3, 5, 2, 6, 1, 7)
    for e in order:
        spread(e).start()
    mine = pl.ds(pl.multiple_of(k * piece, piece), piece)
    total = acc[mine]
    for e in range(1, 8):
        spread(e).wait_recv()
        total = total + r2[e, 0:piece]
    res[core, mine] = total

    def share(e, slot):
        q, row, col = peer(e)
        at = pl.ds(pl.multiple_of(slot * piece, piece), piece)
        return remote(res.at[core, at], res.at[core, at], s3.at[e], v3.at[e], row, col)

    for e in order:
        share(e, k).start()
    for e in range(1, 8):
        share(e, (k + 8 - e) % 8).wait_recv()
    last = remote(res.at[core, pl.ds(0, half)], res.at[core, pl.ds(0, half)], s4, v4, z, partner)
    if both:
        last.start()
        remote(res.at[1 - core, pl.ds(0, half)], res.at[1 - core, pl.ds(0, half)], s4, v4, z, partner).wait_recv()
    one.wait_send()
    for e in range(1, 8):
        spread(e).wait_send()
        share(e, k).wait_send()
    if both:
        last.wait_send()


def pack_gram(mats, precision, gp):
    for o in range(2):
        g = lax.dot_general(mats[o], mats[o], (((0,), (0,)), ((), ())), precision=precision, preferred_element_type=jnp.float32)
        gp[o, 0:128] = g[0:128, 0:128]
        gp[o, 128:256] = g[0:128, 128:256]
        gp[o, 256:384] = g[128:256, 128:256]


def body(lop, lx, rop, rx, xl_out, hl_out, xr_out, hr_out, lv, rv, xl, xr, yl, yr, s, w, other, wsems, *rest):
    names = iter(rest)

    def take(n):
        return [next(names) for _ in range(n)]

    xb, obuf, xcol = take(3), take(3), take(3)
    gsems = take(3)
    dsend, drecv, ysend, yrecv = take(3), take(3), take(3), take(3)
    ssems = take(4)
    bufs = {"gather": (xb, obuf, xcol, *gsems), "scatter": (dsend, drecv, ysend, yrecv, *ssems), "sum": take(13)}
    (lsem,) = take(1)
    loads = [pltpu.make_async_copy(lop, lv, lsem.at[0]), pltpu.make_async_copy(rop, rv, lsem.at[1])]
    for load in loads:
        load.start()
    xs, ys, ops = (xl, xr), (yl, yr), (lv, rv)
    scales = [1.0 / (16 * ref.shape[0]) for ref in xs]
    xl[...] = lx[...]
    xr[...] = rx[...]
    entry_barrier()
    for load in loads:
        load.wait()

    gp, res = bufs["sum"][0], bufs["sum"][4]
    z, c, y, core = place()

    def half_step(phase, carry):
        @pl.when(phase == 0)
        def _():
            pack_gram([r[...].astype(jnp.bfloat16) for r in ys], None, gp)

        @pl.when(phase == 1)
        def _():
            pack_gram([r[...] for r in ys], HI, gp)

        all_sum(384, bufs, False)
        scale = jnp.where(core == 0, scales[0], scales[1])
        s[0:128, 0:128] = res[core, 0:128] * scale
        s[0:128, 128:256] = res[core, 128:256] * scale
        s[128:256, 128:256] = res[core, 256:384] * scale
        chol_inverse(s, w)
        swap = remote(w, other, wsems.at[0], wsems.at[1], z, 2 * y + 1 - core)
        swap.start()
        swap.wait_recv()
        for o in range(2):
            ys[o][...] = dot_hi(ys[o][...], jnp.where(core == o, w[...], other[...]), ((1,), (1,)))
        swap.wait_send()
        return carry

    def sweep(i, carry):
        product(ops, xs, ys, bufs)
        lax.fori_loop(0, 2, half_step, 0)
        for o in range(2):
            xs[o][...] = ys[o][...]
        return carry

    lax.fori_loop(0, SWEEPS, sweep, 0)
    product(ops, xs, ys, bufs)
    for o in range(2):
        h = dot_hi(xs[o][...], ys[o][...], ((0,), (0,)))
        gp[o, 0:256] = h[:, 0:128]
        gp[o, 256:512] = h[:, 128:256]
    all_sum(512, bufs, True)
    for o, out in enumerate((hl_out, hr_out)):
        out[:, 0:128] = res[o, 0:256] * scales[o]
        out[:, 128:256] = res[o, 256:512] * scales[o]
    xl_out[...] = xl[...]
    xr_out[...] = xr[...]


def solution(mesh):
    f32, bf16 = jnp.float32, jnp.bfloat16

    def local_program(left_op, left_start, right_op, right_start):
        nl, nr = left_start.shape[0], right_start.shape[0]
        vm = pl.BlockSpec(memory_space=pltpu.VMEM)
        hbm = pl.BlockSpec(memory_space=pl.ANY)
        dma = pltpu.SemaphoreType.DMA

        def pair(shape, dtype):
            return [pltpu.VMEM(shape(nl), dtype), pltpu.VMEM(shape(nr), dtype)]

        def units(lead, dtype):
            return [pltpu.VMEM(lead + tail, dtype) for tail in ((nr, 256), (nl, 128), (nl, 128))]

        scratch = [pltpu.VMEM(left_op.shape, bf16), pltpu.VMEM(right_op.shape, bf16)]
        scratch += pair(lambda n: (n, 256), f32) + pair(lambda n: (n, 256), f32)
        scratch += [pltpu.VMEM((256, 256), f32)] * 3 + [dma((2,))]
        for lead in ((), (), (4,)):
            scratch += units(lead, bf16)
        scratch += [dma((3, 11)), dma((3, 4)), dma((3,))]
        for lead in ((2, 2), (2,), (), ()):
            scratch += units(lead, f32)
        scratch += [dma((3, 2)), dma((3, 2)), dma((3,)), dma((3,))]
        scratch += [pltpu.VMEM((2, 512, 128), f32), pltpu.VMEM((512, 128), f32), pltpu.VMEM((512, 128), f32), pltpu.VMEM((8, 64, 128), f32), pltpu.VMEM((2, 512, 128), f32)]
        scratch += [dma, dma((8,)), dma((8,)), dma, dma, dma((8,)), dma((8,)), dma]
        scratch += [dma((2,))]
        small = jax.ShapeDtypeStruct((256, 256), f32)
        xl, hl, xr, hr = pl.pallas_call(
            body,
            out_shape=(jax.ShapeDtypeStruct((nl, 256), f32), small, jax.ShapeDtypeStruct((nr, 256), f32), small),
            in_specs=[hbm, vm, hbm, vm],
            out_specs=(vm, vm, vm, vm),
            scratch_shapes=scratch,
            compiler_params=pltpu.CompilerParams(collective_id=0, has_side_effects=True, vmem_limit_bytes=60 * 1024 * 1024),
        )(left_op, left_start, right_op, right_start)
        return xl, hl, xr, hr

    op_spec = P(("batch", "row"), "col")
    vec_spec = P(("batch", "row", "col"), None)
    small_spec = P("batch", None)
    return jax.shard_map(local_program, mesh=mesh, in_specs=(op_spec, vec_spec, op_spec, vec_spec), out_specs=(vec_spec, small_spec, vec_spec, small_spec), check_vma=False)
```

```python
import jax
import jax.numpy as jnp
from jax import lax
from jax.experimental import pallas as pl
from jax.experimental.pallas import tpu as pltpu
from jax.sharding import PartitionSpec as P

SWEEPS = 4
MESH = pl.DeviceIdType.MESH
HI = lax.Precision.HIGHEST
NB = 32


def dot_hi(a, b, dims):
    return lax.dot_general(a, b, (dims, ((), ())), precision=HI, preferred_element_type=jnp.float32)


def diag_block(blk, lane0):
    lane = lax.broadcasted_iota(jnp.int32, (NB, 128), 1)
    row = lax.broadcasted_iota(jnp.int32, (NB, 128), 0)
    groups = NB // 8
    cols = []
    for g in range(groups):
        r0 = 8 * g
        cols.append(jnp.stack([
            jnp.broadcast_to(blk[r0:, lane0 + k:lane0 + k + 1], (NB - r0, 128)) for k in range(r0, r0 + 8)]))
    w = jnp.where(lane % NB == row, 1.0, 0.0)
    piv = []
    for j in range(NB):
        g0, jj = divmod(j, 8)
        r0 = 8 * g0
        u = cols[g0][0]
        p = u[jj:jj + 1]
        piv.append(p)
        if j == NB - 1:
            break
        m = jnp.where(row[r0:] > j, u * (1.0 / p), 0.0)
        if jj < 7:
            cols[g0] = cols[g0][1:] - m[None] * u[jj + 1:8][:, None, :]
        for g in range(g0 + 1, groups):
            d = 8 * (g - g0)
            cols[g] = cols[g] - m[d:][None] * u[d:d + 8][:, None, :]
        w_low = w[r0:] - m * w[j:j + 1]
        w = w_low if g0 == 0 else jnp.concatenate([w[:r0], w_low], axis=0)
    return w * lax.rsqrt(jnp.concatenate(piv, axis=0))


def chol_inverse(s, w):
    rowi = lax.broadcasted_iota(jnp.int32, (256, 256), 0)
    lanei = lax.broadcasted_iota(jnp.int32, (256, 256), 1)
    w[...] = jnp.where(rowi == lanei, 1.0, 0.0)
    for h in range(2):
        base = 128 * h
        for b in range(4):
            r0 = base + NB * b
            rows = slice(r0, r0 + NB)
            li = diag_block(s[rows, base:base + 128], NB * b)
            pan = dot_hi(li[:, :NB], jnp.concatenate([s[rows, base:256], w[rows, 0:base + 128]], axis=1), ((1,), (0,)))
            ns = 256 - base
            s[rows, base:256] = pan[:, :ns]
            w[rows, 0:base + 128] = pan[:, ns:]
            if b < 3:
                upd = dot_hi(pan[:, 0:128].T[NB * (b + 1):], pan, ((1,), (0,)))
                rest = slice(r0 + NB, base + 128)
                s[rest, base:256] = s[rest, base:256] - upd[:, :ns]
                w[rest, 0:base + 128] = w[rest, 0:base + 128] - upd[:, ns:]
        if h == 0:
            pb = s[0:128, 128:256]
            upd = dot_hi(pb.T, jnp.concatenate([pb, w[0:128, 0:128]], axis=1), ((1,), (0,)))
            s[128:256, 128:256] = s[128:256, 128:256] - upd[:, :128]
            w[128:256, 0:128] = w[128:256, 0:128] - upd[:, 128:]


def remote(src, dst, send_sem, recv_sem, row, col):
    return pltpu.make_async_remote_copy(src_ref=src, dst_ref=dst, send_sem=send_sem, recv_sem=recv_sem, device_id={"row": row, "col": col}, device_id_type=MESH)


def place():
    z = lax.axis_index("row")
    c = lax.axis_index("col")
    return z, c, c // 2, c % 2


def entry_barrier():
    z, c, y, core = place()
    barrier = pltpu.get_barrier_semaphore()
    peers = []
    k = z * 2 + y
    for e in range(1, 8):
        q = (k + e) % 8
        peers.append((q // 2, (q % 2) * 2 + core))
    peers.append((z, 2 * y + 1 - core))
    peers.append((z, 2 * (1 - y) + 1 - core))
    for row, col in peers:
        pl.semaphore_signal(barrier, inc=1, device_id={"row": row, "col": col}, device_id_type=MESH)
    pl.semaphore_wait(barrier, len(peers))


def product(ops, xs, ys, bufs):
    z, c, y, core = place()
    xb, obuf, xcol, ss, rr, orr = bufs["gather"]
    dsend, drecv, ysend, yrecv, ds, dr_sem, yss, yrs = bufs["scatter"]
    partner = 2 * y + 1 - core
    across = 2 * (1 - y) + core
    units = ((1, 0, 256), (0, 0, 128), (0, 128, 256))
    t = z + y * (3 - 2 * z)
    kind = core + y * (1 - 2 * core)
    home = t == kind
    step = 1 - 2 * y
    ahead, back = (z + step + 4) % 4, (z - step + 4) % 4
    slots = (c, partner, 2 * (1 - y), 2 * (1 - y) + 1)
    inner = jnp.where(t == 3, 0, 1)
    target = 2 * (1 - y) + jnp.where(y == 1, inner, 1 - inner)

    def goes_ahead(i):
        return ((kind == 0) & (t < 3)) | ((kind == 1) & (t >= 1) & (t < 3) & (i < 2))

    goes_back = (kind == 1) & (t == 1)

    def pass_on(u, i, way):
        at = xcol[u].at[slots[i]]
        return remote(at, at, ss.at[u, 4 * way + i], rr.at[u, slots[i]], back if way else ahead, c)

    def start_passes(u, i):
        @pl.when(goes_ahead(i))
        def _():
            pass_on(u, i, 0).start()

        @pl.when(goes_back)
        def _():
            pass_on(u, i, 1).start()

    def to_partner(u):
        return remote(xb[u], xcol[u].at[c], ss.at[u, 8], rr.at[u, c], z, partner)

    gives = (t == 1 - kind) & (t < 2)

    def cross(u, src):
        return remote(src, xcol[u].at[c], ss.at[u, 9], rr.at[u, c], z, target)

    def ride(u, src):
        return remote(src, obuf[u], ss.at[u, 10], orr.at[u], back, c)

    def arrived(u, i):
        remote(xb[u], xcol[u].at[slots[i]], ss.at[u, 9], rr.at[u, slots[i]], z, target).wait_recv()

    def own(u):
        o, c0, c1 = units[u]
        xb[u][...] = xs[o][:, c0:c1].astype(jnp.bfloat16)

        @pl.when(t >= 2)
        def _():
            cross(u, xb[u]).start()

        @pl.when(t == 2)
        def _():
            ride(u, xb[u]).start()

        @pl.when(gives)
        def _():
            to_partner(u).start()

        @pl.when(home)
        def _():
            xcol[u][c] = xb[u][...]
            start_passes(u, 0)

    def stage(u, i, who=True):
        @pl.when((goes_ahead(i) | goes_back) & who)
        def _():
            if i == 0:
                @pl.when(jnp.logical_not(home))
                def _():
                    arrived(u, 0)
                    start_passes(u, 0)
            else:
                arrived(u, i)
                start_passes(u, i)

    def transit(u, at):
        @pl.when(t == at)
        def _():
            ride(u, xb[u]).wait_recv()
            if at == 1:
                ride(u, obuf[u]).start()
            cross(u, obuf[u]).start()

    def d2d(u, i):
        return remote(dsend[u].at[i, 1 - core], drecv[u].at[i], ds.at[u, i], dr_sem.at[u, i], z, partner)

    def yhop(u):
        return remote(ysend[u], yrecv[u], yss.at[u], yrs.at[u], z, across)

    def compute(u):
        o, c0, c1 = units[u]
        for i in range(4):
            @pl.when(jnp.logical_not(goes_ahead(i) | goes_back))
            def _():
                arrived(u, i)

        n = xs[o].shape[0]
        def half_rows(i, of):
            rows = ops[o][pl.ds(pl.multiple_of(of * 2 * n, 2 * n), 2 * n), :]
            full = xcol[u][...].reshape(4 * n, c1 - c0)
            dsend[u][i] = jnp.dot(rows, full, preferred_element_type=jnp.float32).reshape(2, n, c1 - c0)
            d2d(u, i).start()

        half_rows(0, 1 - y)
        half_rows(1, y)
        d2d(u, 0).wait_recv()
        ysend[u][...] = dsend[u][0, core] + drecv[u][0]
        yhop(u).start()
        d2d(u, 1).wait_recv()
        ys[o][:, c0:c1] = dsend[u][1, core] + drecv[u][1]

    own(0)
    own(1)
    stage(0, 0)
    stage(0, 1)
    own(2)
    transit(0, 1)
    stage(0, 2)
    stage(0, 3)
    stage(1, 0)
    stage(1, 1)
    transit(1, 1)
    stage(1, 2)
    stage(1, 3)
    for i in range(4):
        stage(2, i, t == 0)
    transit(0, 0)
    transit(1, 0)
    compute(0)
    stage(2, 0, t > 0)
    stage(2, 1, t > 0)
    transit(2, 1)
    stage(2, 2, t > 0)
    stage(2, 3, t > 0)
    transit(2, 0)
    compute(1)
    compute(2)
    for u, (o, c0, c1) in enumerate(units):
        yhop(u).wait_recv()
        ys[o][:, c0:c1] = ys[o][:, c0:c1] + yrecv[u][...]
    for u in range(3):
        yhop(u).wait_send()
        for i in range(2):
            d2d(u, i).wait_send()
        for i in range(4):
            @pl.when(goes_ahead(i))
            def _():
                pass_on(u, i, 0).wait_send()

            @pl.when(goes_back)
            def _():
                pass_on(u, i, 1).wait_send()

        @pl.when(gives)
        def _():
            to_partner(u).wait_send()

        cross(u, xb[u]).wait_send()

        @pl.when((t == 1) | (t == 2))
        def _():
            ride(u, xb[u]).wait_send()


def all_sum(half, bufs, gram):
    z, c, y, core = place()
    gp, r1, acc, r2, res, diag, s1, s2, s3, s4, s5, v1, v2, v3, v4, v5 = bufs["sum"]
    partner = 2 * y + 1 - core
    piece = half // 8
    k = z * 2 + y

    def peer(e):
        q = (k + e) % 8
        return q, q // 2, (q % 2) * 2 + core

    rows = half + 8 if gram else half
    one = remote(gp.at[1 - core, pl.ds(0, rows)], r1.at[pl.ds(0, rows)], s1, v1, z, partner)
    one.start()
    one.wait_recv()
    acc[0:rows] = gp[core, 0:rows] + r1[0:rows]

    def spread(e):
        q, row, col = peer(e)
        return remote(acc.at[pl.ds(pl.multiple_of(q * piece, piece), piece)], r2.at[e, pl.ds(0, piece)], s2.at[e], v2.at[e], row, col)

    def spread_diag(e):
        q, row, col = peer(e)
        return remote(acc.at[pl.ds(half, 8)], diag.at[k], s5.at[e], v5.at[e], row, col)

    order = (4, 3, 5, 2, 6, 1, 7)
    for e in order:
        spread(e).start()
        if gram:
            spread_diag(e).start()
    if gram:
        diag[k] = acc[half:half + 8]
    mine = pl.ds(pl.multiple_of(k * piece, piece), piece)
    total = acc[mine]
    for e in range(1, 8):
        spread(e).wait_recv()
        total = total + r2[e, 0:piece]
    res[core, mine] = total
    if gram:
        for e in range(1, 8):
            frm = (k + 8 - e) % 8
            remote(acc.at[pl.ds(half, 8)], diag.at[frm], s5.at[e], v5.at[e], z, partner).wait_recv()
        line = diag[0]
        for q in range(1, 8):
            line = line + diag[q]
        res[core, half:half + 8] = line

    def share(e, slot):
        q, row, col = peer(e)
        at = pl.ds(pl.multiple_of(slot * piece, piece), piece)
        return remote(res.at[core, at], res.at[core, at], s3.at[e], v3.at[e], row, col)

    for e in order:
        share(e, k).start()
    for e in range(1, 8):
        share(e, (k + 8 - e) % 8).wait_recv()
    last = remote(res.at[core, pl.ds(0, half)], res.at[core, pl.ds(0, half)], s4, v4, z, partner)
    if not gram:
        last.start()
        remote(res.at[1 - core, pl.ds(0, half)], res.at[1 - core, pl.ds(0, half)], s4, v4, z, partner).wait_recv()
    one.wait_send()
    for e in range(1, 8):
        spread(e).wait_send()
        share(e, k).wait_send()
        if gram:
            spread_diag(e).wait_send()
    if not gram:
        last.wait_send()


def triangle():
    row = lax.broadcasted_iota(jnp.int32, (128, 128), 0)
    lane = lax.broadcasted_iota(jnp.int32, (128, 128), 1)
    return row <= lane, row == lane


def pack_gram(mats, precision, gp):
    above, on = triangle()
    for o in range(2):
        g = lax.dot_general(mats[o], mats[o], (((0,), (0,)), ((), ())), precision=precision, preferred_element_type=jnp.float32)
        low = g[128:256, 128:256]
        gp[o, 0:128] = jnp.where(above, g[0:128, 0:128], low)
        gp[o, 128:256] = g[0:128, 128:256]
        gp[o, 256:264] = jnp.broadcast_to(jnp.sum(jnp.where(on, low, 0.0), axis=0, keepdims=True), (8, 128))


def body(lop, lx, rop, rx, xl_out, hl_out, xr_out, hr_out, lv, rv, xl, xr, yl, yr, s, w, other, wsems, *rest):
    names = iter(rest)

    def take(n):
        return [next(names) for _ in range(n)]

    xb, obuf, xcol = take(3), take(3), take(3)
    gsems = take(3)
    dsend, drecv, ysend, yrecv = take(3), take(3), take(3), take(3)
    ssems = take(4)
    bufs = {"gather": (xb, obuf, xcol, *gsems), "scatter": (dsend, drecv, ysend, yrecv, *ssems), "sum": take(16)}
    (lsem,) = take(1)
    loads = [pltpu.make_async_copy(lop, lv, lsem.at[0]), pltpu.make_async_copy(rop, rv, lsem.at[1])]
    for load in loads:
        load.start()
    xs, ys, ops = (xl, xr), (yl, yr), (lv, rv)
    scales = [1.0 / (16 * ref.shape[0]) for ref in xs]
    xl[...] = lx[...]
    xr[...] = rx[...]
    entry_barrier()
    for load in loads:
        load.wait()

    gp, res = bufs["sum"][0], bufs["sum"][4]
    z, c, y, core = place()

    def half_step(phase, carry):
        @pl.when(phase == 0)
        def _():
            pack_gram([r[...].astype(jnp.bfloat16) for r in ys], None, gp)

        @pl.when(phase == 1)
        def _():
            pack_gram([r[...] for r in ys], HI, gp)

        all_sum(256, bufs, True)
        scale = jnp.where(core == 0, scales[0], scales[1])
        above, on = triangle()
        tile = res[core, 0:128] * scale
        flip = tile.T
        s[0:128, 0:128] = jnp.where(above, tile, flip)
        s[0:128, 128:256] = res[core, 128:256] * scale
        s[128:256, 128:256] = jnp.where(on, res[core, 256:257] * scale, jnp.where(above, flip, tile))
        chol_inverse(s, w)
        swap = remote(w, other, wsems.at[0], wsems.at[1], z, 2 * y + 1 - core)
        swap.start()
        swap.wait_recv()
        for o in range(2):
            ys[o][...] = dot_hi(ys[o][...], jnp.where(core == o, w[...], other[...]), ((1,), (1,)))
        swap.wait_send()
        return carry

    def sweep(i, carry):
        product(ops, xs, ys, bufs)
        lax.fori_loop(0, 2, half_step, 0)
        for o in range(2):
            xs[o][...] = ys[o][...]
        return carry

    lax.fori_loop(0, SWEEPS, sweep, 0)
    product(ops, xs, ys, bufs)
    for o in range(2):
        h = dot_hi(xs[o][...], ys[o][...], ((0,), (0,)))
        gp[o, 0:256] = h[:, 0:128]
        gp[o, 256:512] = h[:, 128:256]
    all_sum(512, bufs, False)
    for o, out in enumerate((hl_out, hr_out)):
        out[:, 0:128] = res[o, 0:256] * scales[o]
        out[:, 128:256] = res[o, 256:512] * scales[o]
    xl_out[...] = xl[...]
    xr_out[...] = xr[...]


def solution(mesh):
    f32, bf16 = jnp.float32, jnp.bfloat16

    def local_program(left_op, left_start, right_op, right_start):
        nl, nr = left_start.shape[0], right_start.shape[0]
        vm = pl.BlockSpec(memory_space=pltpu.VMEM)
        hbm = pl.BlockSpec(memory_space=pl.ANY)
        dma = pltpu.SemaphoreType.DMA

        def pair(shape, dtype):
            return [pltpu.VMEM(shape(nl), dtype), pltpu.VMEM(shape(nr), dtype)]

        def units(lead, dtype):
            return [pltpu.VMEM(lead + tail, dtype) for tail in ((nr, 256), (nl, 128), (nl, 128))]

        scratch = [pltpu.VMEM(left_op.shape, bf16), pltpu.VMEM(right_op.shape, bf16)]
        scratch += pair(lambda n: (n, 256), f32) + pair(lambda n: (n, 256), f32)
        scratch += [pltpu.VMEM((256, 256), f32)] * 3 + [dma((2,))]
        for lead in ((), (), (4,)):
            scratch += units(lead, bf16)
        scratch += [dma((3, 11)), dma((3, 4)), dma((3,))]
        for lead in ((2, 2), (2,), (), ()):
            scratch += units(lead, f32)
        scratch += [dma((3, 2)), dma((3, 2)), dma((3,)), dma((3,))]
        scratch += [pltpu.VMEM((2, 512, 128), f32), pltpu.VMEM((512, 128), f32), pltpu.VMEM((512, 128), f32), pltpu.VMEM((8, 64, 128), f32), pltpu.VMEM((2, 512, 128), f32), pltpu.VMEM((8, 8, 128), f32)]
        scratch += [dma, dma((8,)), dma((8,)), dma, dma((8,))] * 2
        scratch += [dma((2,))]
        small = jax.ShapeDtypeStruct((256, 256), f32)
        xl, hl, xr, hr = pl.pallas_call(
            body,
            out_shape=(jax.ShapeDtypeStruct((nl, 256), f32), small, jax.ShapeDtypeStruct((nr, 256), f32), small),
            in_specs=[hbm, vm, hbm, vm],
            out_specs=(vm, vm, vm, vm),
            scratch_shapes=scratch,
            compiler_params=pltpu.CompilerParams(collective_id=0, has_side_effects=True, vmem_limit_bytes=60 * 1024 * 1024),
        )(left_op, left_start, right_op, right_start)
        return xl, hl, xr, hr

    op_spec = P(("batch", "row"), "col")
    vec_spec = P(("batch", "row", "col"), None)
    small_spec = P("batch", None)
    return jax.shard_map(local_program, mesh=mesh, in_specs=(op_spec, vec_spec, op_spec, vec_spec), out_specs=(vec_spec, small_spec, vec_spec, small_spec), check_vma=False)
```

```python
import jax
import jax.numpy as jnp
from jax import lax
from jax.experimental import pallas as pl
from jax.experimental.pallas import tpu as pltpu
from jax.sharding import PartitionSpec as P

SWEEPS = 4
MESH = pl.DeviceIdType.MESH
HI = lax.Precision.HIGHEST
NB = 32


def dot_hi(a, b, dims):
    return lax.dot_general(a, b, (dims, ((), ())), precision=HI, preferred_element_type=jnp.float32)


def diag_block(blk, lane0):
    lane = lax.broadcasted_iota(jnp.int32, (NB, 128), 1)
    row = lax.broadcasted_iota(jnp.int32, (NB, 128), 0)
    groups = NB // 8
    cols = []
    for g in range(groups):
        r0 = 8 * g
        cols.append(jnp.stack([
            jnp.broadcast_to(blk[r0:, lane0 + k:lane0 + k + 1], (NB - r0, 128)) for k in range(r0, r0 + 8)]))
    w = jnp.where(lane % NB == row, 1.0, 0.0)
    piv = []
    for j in range(NB):
        g0, jj = divmod(j, 8)
        r0 = 8 * g0
        u = cols[g0][0]
        p = u[jj:jj + 1]
        piv.append(p)
        if j == NB - 1:
            break
        m = jnp.where(row[r0:] > j, u * (1.0 / p), 0.0)
        if jj < 7:
            cols[g0] = cols[g0][1:] - m[None] * u[jj + 1:8][:, None, :]
        for g in range(g0 + 1, groups):
            d = 8 * (g - g0)
            cols[g] = cols[g] - m[d:][None] * u[d:d + 8][:, None, :]
        w_low = w[r0:] - m * w[j:j + 1]
        w = w_low if g0 == 0 else jnp.concatenate([w[:r0], w_low], axis=0)
    return w * lax.rsqrt(jnp.concatenate(piv, axis=0))


def chol_inverse(s, w):
    rowi = lax.broadcasted_iota(jnp.int32, (256, 256), 0)
    lanei = lax.broadcasted_iota(jnp.int32, (256, 256), 1)
    w[...] = jnp.where(rowi == lanei, 1.0, 0.0)
    for h in range(2):
        base = 128 * h
        for b in range(4):
            r0 = base + NB * b
            rows = slice(r0, r0 + NB)
            li = diag_block(s[rows, base:base + 128], NB * b)
            pan = dot_hi(li[:, :NB], jnp.concatenate([s[rows, base:256], w[rows, 0:base + 128]], axis=1), ((1,), (0,)))
            ns = 256 - base
            s[rows, base:256] = pan[:, :ns]
            w[rows, 0:base + 128] = pan[:, ns:]
            if b < 3:
                upd = dot_hi(pan[:, 0:128].T[NB * (b + 1):], pan, ((1,), (0,)))
                rest = slice(r0 + NB, base + 128)
                s[rest, base:256] = s[rest, base:256] - upd[:, :ns]
                w[rest, 0:base + 128] = w[rest, 0:base + 128] - upd[:, ns:]
        if h == 0:
            pb = s[0:128, 128:256]
            upd = dot_hi(pb.T, jnp.concatenate([pb, w[0:128, 0:128]], axis=1), ((1,), (0,)))
            s[128:256, 128:256] = s[128:256, 128:256] - upd[:, :128]
            w[128:256, 0:128] = w[128:256, 0:128] - upd[:, 128:]


def remote(src, dst, send_sem, recv_sem, row, col):
    return pltpu.make_async_remote_copy(src_ref=src, dst_ref=dst, send_sem=send_sem, recv_sem=recv_sem, device_id={"row": row, "col": col}, device_id_type=MESH)


def place():
    z = lax.axis_index("row")
    c = lax.axis_index("col")
    return z, c, c // 2, c % 2


def entry_barrier():
    z, c, y, core = place()
    barrier = pltpu.get_barrier_semaphore()
    peers = []
    k = z * 2 + y
    for e in range(1, 8):
        q = (k + e) % 8
        peers.append((q // 2, (q % 2) * 2 + core))
    peers.append((z, 2 * y + 1 - core))
    peers.append((z, 2 * (1 - y) + 1 - core))
    for row, col in peers:
        pl.semaphore_signal(barrier, inc=1, device_id={"row": row, "col": col}, device_id_type=MESH)
    pl.semaphore_wait(barrier, len(peers))


def product(ops, xs, ys, bufs):
    z, c, y, core = place()
    xb, obuf, xcol, ss, rr, orr = bufs["gather"]
    dsend, drecv, ysend, yrecv, ds, dr_sem, yss, yrs = bufs["scatter"]
    partner = 2 * y + 1 - core
    across = 2 * (1 - y) + core
    units = ((1, 0, 256), (0, 0, 128), (0, 128, 256))
    t = z + y * (3 - 2 * z)
    kind = core + y * (1 - 2 * core)
    home = t == kind
    step = 1 - 2 * y
    ahead, back = (z + step + 4) % 4, (z - step + 4) % 4
    slots = (c, partner, 2 * (1 - y), 2 * (1 - y) + 1)
    inner = jnp.where(t == 3, 0, 1)
    target = 2 * (1 - y) + jnp.where(y == 1, inner, 1 - inner)

    def goes_ahead(i):
        return ((kind == 0) & (t < 3)) | ((kind == 1) & (t >= 1) & (t < 3) & (i < 2))

    goes_back = (kind == 1) & (t == 1)

    def pass_on(u, i, way):
        at = xcol[u].at[slots[i]]
        return remote(at, at, ss.at[u, 4 * way + i], rr.at[u, slots[i]], back if way else ahead, c)

    def start_passes(u, i):
        @pl.when(goes_ahead(i))
        def _():
            pass_on(u, i, 0).start()

        @pl.when(goes_back)
        def _():
            pass_on(u, i, 1).start()

    def to_partner(u):
        return remote(xb[u], xcol[u].at[c], ss.at[u, 8], rr.at[u, c], z, partner)

    gives = (t == 1 - kind) & (t < 2)

    def cross(u, src):
        return remote(src, xcol[u].at[c], ss.at[u, 9], rr.at[u, c], z, target)

    def ride(u, src):
        return remote(src, obuf[u], ss.at[u, 10], orr.at[u], back, c)

    def arrived(u, i):
        remote(xb[u], xcol[u].at[slots[i]], ss.at[u, 9], rr.at[u, slots[i]], z, target).wait_recv()

    def own(u):
        o, c0, c1 = units[u]
        xb[u][...] = xs[o][:, c0:c1].astype(jnp.bfloat16)

        @pl.when(t >= 2)
        def _():
            cross(u, xb[u]).start()

        @pl.when(t == 2)
        def _():
            ride(u, xb[u]).start()

        @pl.when(gives)
        def _():
            to_partner(u).start()

        @pl.when(home)
        def _():
            xcol[u][c] = xb[u][...]
            start_passes(u, 0)

    def stage(u, i, who=True):
        @pl.when((goes_ahead(i) | goes_back) & who)
        def _():
            if i == 0:
                @pl.when(jnp.logical_not(home))
                def _():
                    arrived(u, 0)
                    start_passes(u, 0)
            else:
                arrived(u, i)
                start_passes(u, i)

    def transit(u, at):
        @pl.when(t == at)
        def _():
            ride(u, xb[u]).wait_recv()
            if at == 1:
                ride(u, obuf[u]).start()
            cross(u, obuf[u]).start()

    def d2d(u, i):
        return remote(dsend[u].at[i, 1 - core], drecv[u].at[i], ds.at[u, i], dr_sem.at[u, i], z, partner)

    def yhop(u):
        return remote(ysend[u], yrecv[u], yss.at[u], yrs.at[u], z, across)

    def compute(u):
        o, c0, c1 = units[u]
        for i in range(4):
            @pl.when(jnp.logical_not(goes_ahead(i) | goes_back))
            def _():
                arrived(u, i)

        n = xs[o].shape[0]
        def quarter(q):
            rows = ops[o][pl.ds(pl.multiple_of(q * n, n), n), :]
            return jnp.dot(rows, xcol[u][...].reshape(4 * n, c1 - c0), preferred_element_type=jnp.float32)

        def half_rows(i, of):
            rows = ops[o][pl.ds(pl.multiple_of(of * 2 * n, 2 * n), 2 * n), :]
            full = xcol[u][...].reshape(4 * n, c1 - c0)
            dsend[u][i] = jnp.dot(rows, full, preferred_element_type=jnp.float32).reshape(2, n, c1 - c0)
            d2d(u, i).start()

        if u < 2:
            half_rows(0, 1 - y)
            half_rows(1, y)
            d2d(u, 0).wait_recv()
            ysend[u][...] = dsend[u][0, core] + drecv[u][0]
            yhop(u).start()
        else:
            dsend[u][0, 1 - core] = quarter(2 * (1 - y) + 1 - core)
            d2d(u, 0).start()
            far = quarter(2 * (1 - y) + core)
            d2d(u, 0).wait_recv()
            ysend[u][...] = far + drecv[u][0]
            yhop(u).start()
            half_rows(1, y)

    own(0)
    own(1)
    stage(0, 0)
    stage(0, 1)
    own(2)
    transit(0, 1)
    stage(0, 2)
    stage(0, 3)
    stage(1, 0)
    stage(1, 1)
    transit(1, 1)
    stage(1, 2)
    stage(1, 3)
    for i in range(4):
        stage(2, i, t == 0)
    transit(0, 0)
    transit(1, 0)
    compute(0)
    stage(2, 0, t > 0)
    stage(2, 1, t > 0)
    transit(2, 1)
    stage(2, 2, t > 0)
    stage(2, 3, t > 0)
    transit(2, 0)
    compute(1)
    compute(2)
    for u, (o, c0, c1) in enumerate(units):
        d2d(u, 1).wait_recv()
        yhop(u).wait_recv()
        ys[o][:, c0:c1] = dsend[u][1, core] + drecv[u][1] + yrecv[u][...]
    for u in range(3):
        yhop(u).wait_send()
        for i in range(2):
            d2d(u, i).wait_send()
        for i in range(4):
            @pl.when(goes_ahead(i))
            def _():
                pass_on(u, i, 0).wait_send()

            @pl.when(goes_back)
            def _():
                pass_on(u, i, 1).wait_send()

        @pl.when(gives)
        def _():
            to_partner(u).wait_send()

        cross(u, xb[u]).wait_send()

        @pl.when((t == 1) | (t == 2))
        def _():
            ride(u, xb[u]).wait_send()


def all_sum(half, bufs, gram):
    z, c, y, core = place()
    gp, r1, acc, r2, res, diag, s1, s2, s3, s4, s5, v1, v2, v3, v4, v5 = bufs["sum"]
    partner = 2 * y + 1 - core
    piece = half // 8
    k = z * 2 + y

    def peer(e):
        q = (k + e) % 8
        return q, q // 2, (q % 2) * 2 + core

    rows = half + 8 if gram else half
    one = remote(gp.at[1 - core, pl.ds(0, rows)], r1.at[pl.ds(0, rows)], s1, v1, z, partner)
    one.start()
    one.wait_recv()
    acc[0:rows] = gp[core, 0:rows] + r1[0:rows]

    def spread(e):
        q, row, col = peer(e)
        return remote(acc.at[pl.ds(pl.multiple_of(q * piece, piece), piece)], r2.at[e, pl.ds(0, piece)], s2.at[e], v2.at[e], row, col)

    def spread_diag(e):
        q, row, col = peer(e)
        return remote(acc.at[pl.ds(half, 8)], diag.at[k], s5.at[e], v5.at[e], row, col)

    order = (4, 3, 5, 2, 6, 1, 7)
    for e in order:
        spread(e).start()
        if gram:
            spread_diag(e).start()
    if gram:
        diag[k] = acc[half:half + 8]
    mine = pl.ds(pl.multiple_of(k * piece, piece), piece)
    total = acc[mine]
    for e in range(1, 8):
        spread(e).wait_recv()
        total = total + r2[e, 0:piece]
    res[core, mine] = total
    if gram:
        for e in range(1, 8):
            frm = (k + 8 - e) % 8
            remote(acc.at[pl.ds(half, 8)], diag.at[frm], s5.at[e], v5.at[e], z, partner).wait_recv()
        line = diag[0]
        for q in range(1, 8):
            line = line + diag[q]
        res[core, half:half + 8] = line

    def share(e, slot):
        q, row, col = peer(e)
        at = pl.ds(pl.multiple_of(slot * piece, piece), piece)
        return remote(res.at[core, at], res.at[core, at], s3.at[e], v3.at[e], row, col)

    for e in order:
        share(e, k).start()
    for e in range(1, 8):
        share(e, (k + 8 - e) % 8).wait_recv()
    last = remote(res.at[core, pl.ds(0, half)], res.at[core, pl.ds(0, half)], s4, v4, z, partner)
    if not gram:
        last.start()
        remote(res.at[1 - core, pl.ds(0, half)], res.at[1 - core, pl.ds(0, half)], s4, v4, z, partner).wait_recv()
    one.wait_send()
    for e in range(1, 8):
        spread(e).wait_send()
        share(e, k).wait_send()
        if gram:
            spread_diag(e).wait_send()
    if not gram:
        last.wait_send()


def triangle():
    row = lax.broadcasted_iota(jnp.int32, (128, 128), 0)
    lane = lax.broadcasted_iota(jnp.int32, (128, 128), 1)
    return row <= lane, row == lane


def pack_gram(mats, precision, gp):
    above, on = triangle()
    for o in range(2):
        g = lax.dot_general(mats[o], mats[o], (((0,), (0,)), ((), ())), precision=precision, preferred_element_type=jnp.float32)
        low = g[128:256, 128:256]
        gp[o, 0:128] = jnp.where(above, g[0:128, 0:128], low)
        gp[o, 128:256] = g[0:128, 128:256]
        gp[o, 256:264] = jnp.broadcast_to(jnp.sum(jnp.where(on, low, 0.0), axis=0, keepdims=True), (8, 128))


def body(lop, lx, rop, rx, xl_out, hl_out, xr_out, hr_out, lv, rv, xl, xr, yl, yr, s, w, other, wsems, *rest):
    names = iter(rest)

    def take(n):
        return [next(names) for _ in range(n)]

    xb, obuf, xcol = take(3), take(3), take(3)
    gsems = take(3)
    dsend, drecv, ysend, yrecv = take(3), take(3), take(3), take(3)
    ssems = take(4)
    bufs = {"gather": (xb, obuf, xcol, *gsems), "scatter": (dsend, drecv, ysend, yrecv, *ssems), "sum": take(16)}
    (lsem,) = take(1)
    loads = [pltpu.make_async_copy(lop, lv, lsem.at[0]), pltpu.make_async_copy(rop, rv, lsem.at[1])]
    for load in loads:
        load.start()
    xs, ys, ops = (xl, xr), (yl, yr), (lv, rv)
    scales = [1.0 / (16 * ref.shape[0]) for ref in xs]
    xl[...] = lx[...]
    xr[...] = rx[...]
    entry_barrier()
    for load in loads:
        load.wait()

    gp, res = bufs["sum"][0], bufs["sum"][4]
    z, c, y, core = place()

    def half_step(phase, carry):
        @pl.when(phase == 0)
        def _():
            pack_gram([r[...].astype(jnp.bfloat16) for r in ys], None, gp)

        @pl.when(phase == 1)
        def _():
            pack_gram([r[...] for r in ys], HI, gp)

        all_sum(256, bufs, True)
        scale = jnp.where(core == 0, scales[0], scales[1])
        above, on = triangle()
        tile = res[core, 0:128] * scale
        flip = tile.T
        s[0:128, 0:128] = jnp.where(above, tile, flip)
        s[0:128, 128:256] = res[core, 128:256] * scale
        s[128:256, 128:256] = jnp.where(on, res[core, 256:257] * scale, jnp.where(above, flip, tile))
        chol_inverse(s, w)
        swap = remote(w, other, wsems.at[0], wsems.at[1], z, 2 * y + 1 - core)
        swap.start()
        swap.wait_recv()
        for o in range(2):
            ys[o][...] = dot_hi(ys[o][...], jnp.where(core == o, w[...], other[...]), ((1,), (1,)))
        swap.wait_send()
        return carry

    def sweep(i, carry):
        product(ops, xs, ys, bufs)
        lax.fori_loop(0, 2, half_step, 0)
        for o in range(2):
            xs[o][...] = ys[o][...]
        return carry

    lax.fori_loop(0, SWEEPS, sweep, 0)
    product(ops, xs, ys, bufs)
    for o in range(2):
        h = dot_hi(xs[o][...], ys[o][...], ((0,), (0,)))
        gp[o, 0:256] = h[:, 0:128]
        gp[o, 256:512] = h[:, 128:256]
    all_sum(512, bufs, False)
    for o, out in enumerate((hl_out, hr_out)):
        out[:, 0:128] = res[o, 0:256] * scales[o]
        out[:, 128:256] = res[o, 256:512] * scales[o]
    xl_out[...] = xl[...]
    xr_out[...] = xr[...]


def solution(mesh):
    f32, bf16 = jnp.float32, jnp.bfloat16

    def local_program(left_op, left_start, right_op, right_start):
        nl, nr = left_start.shape[0], right_start.shape[0]
        vm = pl.BlockSpec(memory_space=pltpu.VMEM)
        hbm = pl.BlockSpec(memory_space=pl.ANY)
        dma = pltpu.SemaphoreType.DMA

        def pair(shape, dtype):
            return [pltpu.VMEM(shape(nl), dtype), pltpu.VMEM(shape(nr), dtype)]

        def units(lead, dtype):
            return [pltpu.VMEM(lead + tail, dtype) for tail in ((nr, 256), (nl, 128), (nl, 128))]

        scratch = [pltpu.VMEM(left_op.shape, bf16), pltpu.VMEM(right_op.shape, bf16)]
        scratch += pair(lambda n: (n, 256), f32) + pair(lambda n: (n, 256), f32)
        scratch += [pltpu.VMEM((256, 256), f32)] * 3 + [dma((2,))]
        for lead in ((), (), (4,)):
            scratch += units(lead, bf16)
        scratch += [dma((3, 11)), dma((3, 4)), dma((3,))]
        for lead in ((2, 2), (2,), (), ()):
            scratch += units(lead, f32)
        scratch += [dma((3, 2)), dma((3, 2)), dma((3,)), dma((3,))]
        scratch += [pltpu.VMEM((2, 512, 128), f32), pltpu.VMEM((512, 128), f32), pltpu.VMEM((512, 128), f32), pltpu.VMEM((8, 64, 128), f32), pltpu.VMEM((2, 512, 128), f32), pltpu.VMEM((8, 8, 128), f32)]
        scratch += [dma, dma((8,)), dma((8,)), dma, dma((8,))] * 2
        scratch += [dma((2,))]
        small = jax.ShapeDtypeStruct((256, 256), f32)
        xl, hl, xr, hr = pl.pallas_call(
            body,
            out_shape=(jax.ShapeDtypeStruct((nl, 256), f32), small, jax.ShapeDtypeStruct((nr, 256), f32), small),
            in_specs=[hbm, vm, hbm, vm],
            out_specs=(vm, vm, vm, vm),
            scratch_shapes=scratch,
            compiler_params=pltpu.CompilerParams(collective_id=0, has_side_effects=True, vmem_limit_bytes=60 * 1024 * 1024),
        )(left_op, left_start, right_op, right_start)
        return xl, hl, xr, hr

    op_spec = P(("batch", "row"), "col")
    vec_spec = P(("batch", "row", "col"), None)
    small_spec = P("batch", None)
    return jax.shard_map(local_program, mesh=mesh, in_specs=(op_spec, vec_spec, op_spec, vec_spec), out_specs=(vec_spec, small_spec, vec_spec, small_spec), check_vma=False)
```
